128 devices in a mesh: gx: 16 (over y, x), gy: 8 (over z, core).
Axes of the slice: x: 4, y: 4, z: 4, core: 2. Of those that a mesh axis runs over, the one named last changes fastest.
Arguments:
- probes: bfloat16 [512, 2048, 256], P('gx', 'gy'), may hold values from -6 to 6
- blk_rows: int32 [16384, 128], P(('gx', 'gy')), may hold values from 0 to 8191
- blk_sensor: int32 [16384], P(('gx', 'gy')), may hold values from 0 to 1023, as said below
- blk_count: int32 [128], P(('gx', 'gy')), may hold values from 64 to 128, as said below
- coef: bfloat16 [16384, 128], P(('gx', 'gy')), may hold values from -5 to 5
- owner: int32 [1024], replicated, may hold values from 0 to 127, as said below
- weights: float32 [1024], replicated, may hold values from 0.1 to 1
Outputs:
- sensitivity: float32 [1024], P(('gx', 'gy'))
- new_weights: float32 [1024], replicated
- density: float32 [512, 2048], P('gx', 'gy')
The draws below stay inside these ranges and needn't reach their ends.
Inputs may be any that keep to these rules, and one draw needn't show every extreme that they name: `owner`: every device owns exactly 8 sensors. `blk_sensor`: among the live slots of one tile, at most 2 belong to sensors of one owner; in every draw some owner receives 2 live blocks from every tile. `blk_count`: some tile has all 128 slots live.
All inputs are finite; a program needn't handle non-finite values.
Results may differ from the reference program's by a relative error of at most 0.0008.
Values may be sent and summed in bfloat16 or wider, within the bound.
A program may use at most 128 MiB of HBM per device.

```python
import math
import jax
import jax.numpy as jnp
from jax import lax

P_SIZE = 256
FOOT = 128
TR = 32
TC = 256
SPD = 8
CAP = 2
SENSORS = 1024
NBLK = 128
GR = 512
GC = 2048
N_GX = 16
N_GY = 8
DEVICES = 128


def layout(key):
    perm = jax.random.permutation(jax.random.fold_in(key, 11), SENSORS).astype(jnp.int32)
    owners = perm // SPD
    inverse = jnp.argsort(perm, stable=True).astype(jnp.int32)
    hot = jax.random.permutation(jax.random.fold_in(key, 12), DEVICES)[:2].astype(jnp.int32)
    entries = jnp.arange(DEVICES * CAP, dtype=jnp.int32)
    is_hot = jnp.any((entries // CAP)[:, None] == hot[None, :], axis=1).astype(jnp.int32)
    score = jax.random.randint(jax.random.fold_in(key, 13), (DEVICES, DEVICES * CAP), 0, 2 ** 20, dtype=jnp.int32)
    score = (score + is_hot[None, :] * 2 ** 21) * (DEVICES * CAP) + entries[None, :]
    chosen = lax.top_k(score, NBLK)[1].astype(jnp.int32)
    dest = chosen // CAP
    within = jax.random.randint(jax.random.fold_in(key, 14), (DEVICES, NBLK), 0, SPD, dtype=jnp.int32)
    sensor = inverse[dest * SPD + within]
    count = jax.random.randint(jax.random.fold_in(key, 15), (DEVICES,), NBLK // 2, NBLK + 1, dtype=jnp.int32)
    full_tile = jax.random.randint(jax.random.fold_in(key, 16), (), 0, DEVICES, dtype=jnp.int32)
    count = jnp.where(jnp.arange(DEVICES, dtype=jnp.int32) == full_tile, NBLK, count)
    return (owners, sensor.reshape(-1), count)


def draw_owner(key, part):
    return layout(key)[0]


def draw_blk_sensor(key, part):
    return layout(key)[1]


def draw_blk_count(key, part):
    return layout(key)[2]


def touch_ends(values, own_key, least, top_value):
    longest = values.shape.index(max(values.shape))
    spots = []
    for shift in (0, 1):
        where = [jax.random.randint(jax.random.fold_in(own_key, axis), (), 0, length) for axis, length in enumerate(values.shape)]
        where[longest] = (where[longest] + shift) % values.shape[longest]
        spots.append(tuple(where))
    return values.at[spots[0]].set(least).at[spots[1]].set(top_value)


def block_levels(key, dims, shards, smallest, high):
    loudness = 1.0
    for position, blocks in shards:
        steps = jax.random.uniform(jax.random.fold_in(jax.random.fold_in(key, 6), position), (blocks,), jnp.float32, smallest / len(shards), high / len(shards))
        loudness = loudness * jnp.repeat(jnp.exp(steps), dims[position] // blocks).reshape((-1,) + (1,) * (len(dims) - 1 - position))
    return loudness


def normal_values(key, extent, deviation, limit, cuts=(), kind=jnp.bfloat16):
    values = deviation * jax.random.normal(key, extent, jnp.float32)
    if cuts:
        values = values * block_levels(key, extent, cuts, -0.22, 0.18)
    return jnp.clip(values, -limit, limit).astype(kind)


def setup_inputs(seed: int = 0) -> dict:
    keys = jax.random.split(jax.random.key(seed), 8)
    return {
        "probes": normal_values(keys[0], (GR, GC, P_SIZE), 1.0, 6.0, ((0, 16), (1, 8))),
        "blk_rows": touch_ends(jax.random.randint(keys[1], (DEVICES * NBLK, FOOT), 0, TR * TC), jax.random.fold_in(keys[1], 1), 0, (TR * TC) - 1).astype(jnp.int32),
        "blk_sensor": draw_blk_sensor(jax.random.fold_in(keys[7], 71), 0),
        "blk_count": draw_blk_count(jax.random.fold_in(keys[7], 71), 0),
        "coef": normal_values(keys[4], (DEVICES * NBLK, FOOT), 1.0, 5.0, ((0, 128),)),
        "owner": draw_owner(jax.random.fold_in(keys[7], 71), 0),
        "weights": jnp.clip(jnp.exp(jax.random.uniform(keys[6], (SENSORS,), jnp.float32, math.log(0.1), math.log(1.0))), 0.1, 1.0),
    }


def reference(probes, blk_rows, blk_sensor, blk_count, coef, owner, weights):
    tiles = probes.reshape(N_GX, TR, N_GY, TC, P_SIZE).transpose(0, 2, 1, 3, 4).reshape(N_GX * N_GY, TR * TC, P_SIZE)
    rows = blk_rows.reshape(DEVICES, NBLK, FOOT)
    sensors = blk_sensor.reshape(DEVICES, NBLK)
    coefs = coef.reshape(DEVICES, NBLK, FOOT)
    live = (jnp.arange(NBLK, dtype=jnp.int32)[None, :] < blk_count[:, None]).astype(jnp.float32)

    def accumulate(obs, inputs):
        tile, row_ids, sens, weight, alive = inputs
        picked = tile[row_ids.reshape(-1)].reshape(NBLK, FOOT, P_SIZE).astype(jnp.float32)
        contrib = weight.astype(jnp.float32)[:, :, None] * picked * alive[:, None, None]
        return (obs.at[sens].add(contrib), None)
    obs = lax.scan(accumulate, jnp.zeros((SENSORS, FOOT, P_SIZE), jnp.float32), (tiles, rows, sensors, coefs, live))[0]
    sens_h = lax.optimization_barrier(jnp.sum(obs * obs, axis=(1, 2))) / (FOOT * P_SIZE)
    order = jnp.argsort(owner * SENSORS + jnp.arange(SENSORS, dtype=jnp.int32))
    sensitivity = sens_h[order]
    gain = weights * jnp.sqrt(1.0 + sens_h)
    new_weights = SENSORS * gain / jnp.sum(gain)
    values = live[:, :, None] * new_weights[sensors][:, :, None] * jnp.square(coefs.astype(jnp.float32))
    tile_ids = jnp.broadcast_to(jnp.arange(DEVICES, dtype=jnp.int32)[:, None, None], rows.shape)
    dens = jnp.zeros((DEVICES, TR * TC), jnp.float32).at[tile_ids, rows].add(values)
    density = dens.reshape(N_GX, N_GY, TR, TC).transpose(0, 2, 1, 3).reshape(N_GX * TR, N_GY * TC)
    return (sensitivity, new_weights, density)
```

```python
import functools

import jax
import jax.numpy as jnp
from jax import lax
from jax.experimental import pallas as pl
from jax.experimental.pallas import tpu as pltpu
from jax.sharding import PartitionSpec as P

MESH = pl.DeviceIdType.MESH
HIGHEST = lax.Precision.HIGHEST
STRIDE = 37
GROUP = 4
MROWS = 256


def shifted(step):
    off = lax.rem((step + 1) * STRIDE, 128)
    gx, gy = lax.axis_index("gx"), lax.axis_index("gy")
    y = lax.rem(gx // 4 + off // 32, 4)
    x = lax.rem(lax.rem(gx, 4) + lax.rem(off // 8, 4), 4)
    z = lax.rem(gy // 2 + lax.rem(off // 2, 4), 4)
    core = lax.rem(lax.rem(gy, 2) + lax.rem(off, 2), 2)
    return y * 4 + x, z * 2 + core


def kernel(
    rows_s, probes, meta, rows_v, coef_v, ids_v, owner_v, weights_v,
    sens_o, new_o, dens_o,
    tile, stage, send, recv, meta_in, dens, obs, h_send, h_in, h_mid, h_in2, wide,
    data_ss, data_rs, meta_ss, meta_rs, h_ss, h_rs, h2_ss, h2_rs,
):
    n_pts, probe_n = probes.shape
    foot = 128
    gx, gy = lax.axis_index("gx"), lax.axis_index("gy")
    me = gx * 8 + gy

    barrier = pltpu.get_barrier_semaphore()

    def greet(step, c):
        pl.semaphore_signal(barrier, inc=1, device_id=shifted(step), device_id_type=MESH)
        return c

    lax.fori_loop(0, 127, greet, 0)

    def widen(i, c):
        part = pl.ds(pl.multiple_of(i * 64, 64), 64)
        block = probes[part, :].astype(jnp.float32)
        tile[part, 0, :] = block[:, :128]
        tile[part, 1, :] = block[:, 128:]
        return c

    lax.fori_loop(0, n_pts // 64, widen, 0)
    pl.semaphore_wait(barrier, 127)

    def data_copy(step):
        return pltpu.make_async_remote_copy(
            src_ref=send.at[step], dst_ref=recv.at[step],
            send_sem=data_ss.at[step], recv_sem=data_rs.at[step],
            device_id=shifted(step), device_id_type=MESH,
        )

    def meta_copy(step):
        tx, ty = shifted(step)
        return pltpu.make_async_remote_copy(
            src_ref=meta.at[tx * 8 + ty], dst_ref=meta_in.at[step],
            send_sem=meta_ss.at[step], recv_sem=meta_rs.at[step],
            device_id=(tx, ty), device_id_type=MESH,
        )

    def gather(step, c):
        tx, ty = shifted(step)
        base = (tx * 8 + ty) * 128
        for i in range(128):
            stage[i] = tile[rows_s[base + i]]

        @pl.when(step >= 1)
        def _():
            meta_copy(step - 1).start()
            data_copy(step - 1).start()

        send[step, :, :128] = stage[:, 0, :].astype(jnp.bfloat16)
        send[step, :, 128:] = stage[:, 1, :].astype(jnp.bfloat16)
        return c

    lax.fori_loop(0, 128, gather, 0)
    recv[127] = send[127]
    meta_in[127] = meta[me]

    q = lax.broadcasted_iota(jnp.int32, (64, 128), 0)
    hi_of = jnp.where(q < 32, 2 * q, 2 * q - 63)
    lo_of = lax.broadcasted_iota(jnp.int32, (128, 128), 0)

    def spread(slot, c):
        row = rows_v[pl.ds(slot, 1), :]
        val = coef_v[pl.ds(slot, 1), :]
        high = jnp.where(row // 128 == hi_of, val, 0.0).astype(jnp.bfloat16)
        low = jnp.where(lax.rem(row, 128) == lo_of, val, 0.0).astype(jnp.bfloat16)
        dens[slot] = lax.dot_general(
            high, low, (((1,), (1,)), ((), ())), preferred_element_type=jnp.float32
        )
        return c

    lax.fori_loop(0, 128, spread, 0)

    obs[...] = jnp.zeros_like(obs)
    sens_of = lax.broadcasted_iota(jnp.int32, (MROWS, 128), 0).astype(jnp.float32)

    def mix(g, c):
        for k in range(GROUP):
            step = g * GROUP + k

            @pl.when(step < 127)
            def _():
                meta_copy(step).wait_recv()
                data_copy(step).wait_recv()

        cols = jnp.concatenate([recv[g * GROUP + k] for k in range(GROUP)], axis=0)
        for m in range(1024 // MROWS):
            mixer = jnp.concatenate(
                [
                    jnp.where(
                        meta_in[g * GROUP + k, 1:2, :] - float(m * MROWS) == sens_of,
                        meta_in[g * GROUP + k, 0:1, :], 0.0,
                    ).astype(jnp.bfloat16)
                    for k in range(GROUP)
                ],
                axis=1,
            )
            obs[m * MROWS:(m + 1) * MROWS, :] += jnp.dot(
                mixer, cols, preferred_element_type=jnp.float32
            )
        return c

    lax.fori_loop(0, 128 // GROUP, mix, 0)

    ones = jnp.ones((8, 128), jnp.float32)
    for k in range(8):
        part = obs[k * 128:(k + 1) * 128, :]
        part = part * part
        part = part[:, :128] + part[:, 128:]
        h_send[k:k + 1, :] = lax.dot_general(
            ones, part, (((1,), (1,)), ((), ())),
            preferred_element_type=jnp.float32, precision=HIGHEST,
        )[0:1, :] * (1.0 / (foot * probe_n))

    def first_copy(k):
        to = lax.rem(gy + k, 8)
        return pltpu.make_async_remote_copy(
            src_ref=h_send, dst_ref=h_in.at[gy],
            send_sem=h_ss.at[k], recv_sem=h_rs.at[k],
            device_id=(gx, to), device_id_type=MESH,
        )

    def second_copy(k):
        to = lax.rem(gx + k, 16)
        return pltpu.make_async_remote_copy(
            src_ref=h_mid, dst_ref=h_in2.at[gx],
            send_sem=h2_ss.at[k], recv_sem=h2_rs.at[k],
            device_id=(to, gy), device_id_type=MESH,
        )

    for k in range(1, 8):
        first_copy(k).start()
    h_in[gy] = h_send[...]
    mine = owner_v[...] == me
    count = jnp.where(mine, 1.0, 0.0)
    before = jnp.where(
        lax.broadcasted_iota(jnp.int32, (128, 128), 0) < lax.broadcasted_iota(jnp.int32, (128, 128), 1),
        1.0, 0.0,
    )
    above = jnp.where(
        lax.broadcasted_iota(jnp.int32, (8, 8), 1) < lax.broadcasted_iota(jnp.int32, (8, 8), 0),
        1.0, 0.0,
    )
    in_row = jnp.dot(count, before, precision=HIGHEST, preferred_element_type=jnp.float32)
    rank = in_row + jnp.dot(
        above, jnp.broadcast_to(jnp.sum(count, axis=1, keepdims=True), (8, 128)),
        precision=HIGHEST, preferred_element_type=jnp.float32,
    )
    rank = jnp.where(mine, rank, -1.0)
    for k in range(1, 8):
        first_copy(k).wait_recv()
    total = h_in[0]
    for k in range(1, 8):
        total = total + h_in[k]
    h_mid[...] = total
    for k in range(1, 16):
        second_copy(k).start()
    h_in2[gx] = total
    for k in range(1, 16):
        second_copy(k).wait_recv()
    total = h_in2[0]
    for k in range(1, 16):
        total = total + h_in2[k]

    gain = weights_v[...] * jnp.sqrt(1.0 + total)
    new = 1024.0 * gain / jnp.sum(gain)
    new_o[...] = new
    for k in range(8):
        sens_o[k:k + 1, :] = jnp.broadcast_to(
            jnp.sum(jnp.where(rank == float(k), total, 0.0), keepdims=True), (1, 128)
        )

    ids = ids_v[...]
    lane = lax.broadcasted_iota(jnp.int32, (128, 128), 1)
    picked = jnp.zeros((128, 128), jnp.float32)
    for k in range(8):
        picked = picked + jnp.where(ids == lane + k * 128, new_o[k:k + 1, :], 0.0)
    wide[...] = jnp.broadcast_to(jnp.sum(picked, axis=1, keepdims=True), (128, 128))

    def weigh(i, acc):
        for u in range(8):
            slot = i * 8 + u
            acc = acc + wide[pl.ds(slot, 1), :] * dens[slot]
        return acc

    out = lax.fori_loop(0, 16, weigh, jnp.zeros((64, 128), jnp.float32))
    dens_o[:, :128] = out[:32]
    dens_o[:, 128:] = out[32:]

    def drain(step, c):
        meta_copy(step).wait_send()
        data_copy(step).wait_send()
        return c

    lax.fori_loop(0, 127, drain, 0)
    for k in range(1, 8):
        first_copy(k).wait_send()
    for k in range(1, 16):
        second_copy(k).wait_send()


def local(probes, blk_rows, blk_sensor, blk_count, coef, owner, weights):
    tile_r, tile_c, probe_n = probes.shape
    nblk, foot = blk_rows.shape
    alive = jnp.arange(nblk, dtype=jnp.int32) < blk_count[0]
    coef_m = jnp.where(alive[:, None], coef.astype(jnp.float32), 0.0)
    rows_t = blk_rows.T.reshape(-1)
    ids = jnp.broadcast_to(blk_sensor.astype(jnp.float32)[None, :], (foot, nblk))
    meta = jnp.stack([coef_m.T, ids], axis=1)
    ids_v = jnp.broadcast_to(blk_sensor[:, None], (nblk, 128))
    vmem = pl.BlockSpec(memory_space=pltpu.VMEM)
    smem = pl.BlockSpec(memory_space=pltpu.SMEM)
    f32 = jnp.float32
    sens, new, dens = pl.pallas_call(
        kernel,
        out_shape=(
            jax.ShapeDtypeStruct((8, 128), f32),
            jax.ShapeDtypeStruct((8, 128), f32),
            jax.ShapeDtypeStruct((tile_r, tile_c), f32),
        ),
        in_specs=[smem] + [vmem] * 7,
        out_specs=(vmem, vmem, vmem),
        scratch_shapes=[
            pltpu.VMEM((tile_r * tile_c, 2, 128), f32),
            pltpu.VMEM((nblk, 2, 128), f32),
            pltpu.VMEM((128, nblk, probe_n), jnp.bfloat16),
            pltpu.VMEM((128, nblk, probe_n), jnp.bfloat16),
            pltpu.VMEM((128, 2, 128), f32),
            pltpu.VMEM((nblk, 64, 128), f32),
            pltpu.VMEM((1024, probe_n), f32),
            pltpu.VMEM((8, 128), f32),
            pltpu.VMEM((8, 8, 128), f32),
            pltpu.VMEM((8, 128), f32),
            pltpu.VMEM((16, 8, 128), f32),
            pltpu.VMEM((128, 128), f32),
            pltpu.SemaphoreType.DMA((128,)),
            pltpu.SemaphoreType.DMA((128,)),
            pltpu.SemaphoreType.DMA((128,)),
            pltpu.SemaphoreType.DMA((128,)),
            pltpu.SemaphoreType.DMA((8,)),
            pltpu.SemaphoreType.DMA((8,)),
            pltpu.SemaphoreType.DMA((16,)),
            pltpu.SemaphoreType.DMA((16,)),
        ],
        compiler_params=pltpu.CompilerParams(
            collective_id=0, has_side_effects=True, vmem_limit_bytes=60 * 2 ** 20
        ),
        name="exchange",
    )(
        rows_t, probes.reshape(tile_r * tile_c, probe_n), meta, blk_rows, coef_m, ids_v,
        owner.reshape(8, 128), weights.reshape(8, 128),
    )
    return sens[:, 0], new.reshape(-1), dens


def solution(mesh):
    in_specs = (
        P("gx", "gy", None),
        P(("gx", "gy"), None),
        P(("gx", "gy")),
        P(("gx", "gy")),
        P(("gx", "gy"), None),
        P(),
        P(),
    )
    out_specs = (P(("gx", "gy")), P(), P("gx", "gy"))
    return jax.shard_map(local, mesh=mesh, in_specs=in_specs, out_specs=out_specs, check_vma=False)
```

```python
import jax
import jax.numpy as jnp
from jax import lax
from jax.experimental import pallas as pl
from jax.experimental.pallas import tpu as pltpu
from jax.sharding import PartitionSpec as P

MESH = pl.DeviceIdType.MESH
HIGHEST = lax.Precision.HIGHEST
FIRST = (0, 1, 2, 2)
SECOND = (1, 2, 0, 0)
THIRD = (2, 0, 1, 1)


def place():
    gx, gy = lax.axis_index("gx"), lax.axis_index("gy")
    return [lax.rem(gx, 4), gx // 4, gy // 2], lax.rem(gy, 2)


def peer(axis, off, core_off):
    at, core = place()
    at[axis] = lax.rem(at[axis] + off, 4)
    return at[1] * 4 + at[0], at[2] * 2 + lax.rem(core + core_off, 2)


def order(i):
    return lax.rem(1 + 2 * i - 3 * (i // 2), 4)


def decode(pos):
    return order(pos // 8), order(lax.rem(pos, 4)), lax.rem(pos, 8) // 4


def kernel(
    rows_s, probes, meta, rows_v, coef_v, ids_v, owner_v, weights_v,
    sens_o, new_o, dens_o,
    tile, stage, send, zone, metas, dens, part, final, steps_v, h_send, h_in, h_mid, h_in2, wide,
    ss1, rs1, ss2, rs2, ms1, mr1, ms2, mr2, fs, fr, h_ss, h_rs, h2_ss, h2_rs,
):
    n_pts, probe_n = probes.shape
    foot = 128
    gx, gy = lax.axis_index("gx"), lax.axis_index("gy")
    me = gx * 8 + gy
    at, core = place()
    bf16, f32 = jnp.bfloat16, jnp.float32

    barrier = pltpu.get_barrier_semaphore()

    def greet(device):
        pl.semaphore_signal(barrier, inc=1, device_id=device, device_id_type=MESH)

    for k in range(1, 16):
        greet((lax.rem(gx // 4 + k // 4, 4) * 4 + lax.rem(lax.rem(gx, 4) + k % 4, 4), gy))
    for k in range(1, 8):
        greet((gx, lax.rem(gy + k, 8)))
    for axis in (0, 1):
        for off in (1, 2, 3):
            greet(peer(axis, off, 1))

    flat = tile.reshape(2 * n_pts, 128)

    def widen(i, c):
        block = probes[pl.ds(pl.multiple_of(i * 64, 64), 64), :].astype(f32)
        flat[pl.ds(i * 128, 64, 2), :] = block[:, :128]
        flat[pl.ds(i * 128 + 1, 64, 2), :] = block[:, 128:]
        return c

    lax.fori_loop(0, n_pts // 64, widen, 0)
    for i in range(16):
        steps_v[i * 16:(i + 1) * 16, :] = (
            lax.broadcasted_iota(jnp.int32, (16, 128), 0) + i * 16
        ).astype(f32).astype(bf16)
    pl.semaphore_wait(barrier, 28)

    def meta1(k, of, oc):
        first = lax.rem(core + oc, 2) * 64 + k * 16 + lax.rem(at[FIRST[k]] + of, 4) * 4
        src = oc * 4 + of
        return pltpu.make_async_remote_copy(
            src_ref=meta.at[pl.ds(first, 4)], dst_ref=metas.at[k, pl.ds(0, 4), src],
            send_sem=ms1.at[k, src], recv_sem=mr1.at[k, src],
            device_id=peer(FIRST[k], of, oc), device_id_type=MESH,
        )

    def meta2(k, og):
        return pltpu.make_async_remote_copy(
            src_ref=metas.at[k, lax.rem(at[SECOND[k]] + og, 4)], dst_ref=metas.at[k, 4 + og],
            send_sem=ms2.at[k, og], recv_sem=mr2.at[k, og],
            device_id=peer(SECOND[k], og, 0), device_id_type=MESH,
        )

    def copy1(k, pos):
        og, of, oc = decode(pos)
        return pltpu.make_async_remote_copy(
            src_ref=send.at[k, pos], dst_ref=zone.at[k, og + 3 * ((og + 3) // 4), oc * 4 + of],
            send_sem=ss1.at[k, pos], recv_sem=rs1.at[k, pos],
            device_id=peer(FIRST[k], of, oc), device_id_type=MESH,
        )

    def copy2(k, pos):
        og, of, oc = decode(pos)
        return pltpu.make_async_remote_copy(
            src_ref=zone.at[k, 3 + og, oc * 4 + of], dst_ref=zone.at[k, og, oc * 4 + of],
            send_sem=ss2.at[k, pos], recv_sem=rs2.at[k, pos],
            device_id=peer(SECOND[k], og, 0), device_id_type=MESH,
        )

    def copy3(k, oh):
        block = lax.rem(at[THIRD[k]] + oh, 4)
        return pltpu.make_async_remote_copy(
            src_ref=part.at[k, pl.ds(pl.multiple_of(block * 256, 256), 256)], dst_ref=final.at[k, oh - 1],
            send_sem=fs.at[k, oh], recv_sem=fr.at[k, oh],
            device_id=peer(THIRD[k], oh, 0), device_id_type=MESH,
        )

    others = [(of, oc) for oc in (0, 1) for of in (1, 3, 2, 0) if (of, oc) != (0, 0)]
    for of, oc in others:
        for k in range(4):
            meta1(k, of, oc).start()
    for k in range(4):
        metas[k, 0:4, 0] = meta[pl.ds(core * 64 + k * 16 + at[FIRST[k]] * 4, 4)]

    def gather(k, pos, buf):
        og, of, oc = decode(pos)
        chan = (
            lax.rem(core + oc, 2) * 64 + k * 16
            + lax.rem(at[FIRST[k]] + of, 4) * 4 + lax.rem(at[SECOND[k]] + og, 4)
        )
        base = chan * 128
        for i in range(128):
            stage[buf, 2 * i:2 * i + 2, :] = tile[rows_s[base + i]]
        send[k, pos, :, :128] = stage[buf, pl.ds(0, 128, 2), :].astype(bf16)
        send[k, pos, :, 128:] = stage[buf, pl.ds(1, 128, 2), :].astype(bf16)

    def give(k, pos):
        mine = lax.rem(pos, 8) == 3

        @pl.when(mine)
        def _():
            og, _, _ = decode(pos)
            zone[k, og + 3 * ((og + 3) // 4), 0] = send[k, pos]

        @pl.when(jnp.logical_not(mine))
        def _():
            copy1(k, pos).start()

    def first_loop(pos, c):
        gather(0, pos, 0)

        @pl.when(pos > 0)
        def _():
            give(2, pos - 1)

        gather(1, pos, 1)
        give(0, pos)
        gather(2, pos, 2)
        give(1, pos)
        return c

    lax.fori_loop(0, 32, first_loop, 0)

    def second_loop(pos, c):
        gather(3, pos, 0)

        @pl.when(pos == 0)
        def _():
            give(2, 31)

        @pl.when(pos > 0)
        def _():
            give(3, pos - 1)
        return c

    lax.fori_loop(0, 32, second_loop, 0)
    give(3, 31)

    for of, oc in others:
        for k in range(4):
            meta1(k, of, oc).wait_recv()
    for og in (1, 3, 2):
        for k in range(4):
            meta2(k, og).start()

    q = lax.broadcasted_iota(jnp.int32, (64, 128), 0)
    hi_of = jnp.where(q < 32, 2 * q, 2 * q - 63)
    lo_of = lax.broadcasted_iota(jnp.int32, (128, 128), 0)

    def spread(first):
        for u in range(4):
            row = rows_v[pl.ds(first + u, 1), :]
            val = coef_v[pl.ds(first + u, 1), :]
            high = jnp.where(row // 128 == hi_of, val, 0.0).astype(bf16)
            low = jnp.where(lax.rem(row, 128) == lo_of, val, 0.0).astype(bf16)
            dens[first + u] = lax.dot_general(
                high, low, (((1,), (1,)), ((), ())), preferred_element_type=f32
            )

    def forward(k, pos):
        @pl.when(lax.rem(pos, 8) != 3)
        def _():
            copy1(k, pos).wait_recv()

        copy2(k, pos).start()

    def forward_loop(pos, c):
        spread(pos * 4)
        for k in range(3):
            forward(k, pos)
        return c

    lax.fori_loop(0, 24, forward_loop, 0)
    part[...] = jnp.zeros_like(part)

    def mix(k, group):
        pos = group * 4
        og, _, oc = decode(pos)
        for u in range(4):
            @pl.when(pos + u < 24)
            def _():
                copy2(k, pos + u).wait_recv()

            @pl.when(jnp.logical_and(pos + u >= 24, pos + u != 27))
            def _():
                copy1(k, pos + u).wait_recv()

        cols = zone[k, og, pl.ds(oc * 4, 4)].reshape(512, probe_n)
        slot = og + 4 * ((og + 3) // 4) + at[SECOND[k]] * (1 - (og + 3) // 4)
        tags = [metas[k, slot, oc * 4 + u] for u in range(4)]
        vals = [jnp.broadcast_to(t[0:1], (16, 128)).astype(bf16) for t in tags]
        zero = jnp.zeros((16, 128), bf16)
        for m in range(4):
            names = [jnp.broadcast_to(t[1:2] - float(m * 256), (16, 128)).astype(bf16) for t in tags]
            mixer = jnp.concatenate(
                [
                    jnp.concatenate(
                        [
                            jnp.where(names[u] == steps_v[i * 16:(i + 1) * 16, :], vals[u], zero)
                            for i in range(16)
                        ],
                        axis=0,
                    )
                    for u in range(4)
                ],
                axis=1,
            )
            part[k, m * 256:(m + 1) * 256, :] += jnp.dot(mixer, cols, preferred_element_type=f32)

    def late_loop(i, c):
        @pl.when(i == 0)
        def _():
            for og in (1, 3, 2):
                for k in range(4):
                    meta2(k, og).wait_recv()

        spread(96 + i * 4)
        for u in range(3):
            forward(3, i * 3 + u)
        mix(0, lax.rem(i + 6, 8))
        return c

    lax.fori_loop(0, 8, late_loop, 0)
    for oh in (1, 3, 2):
        copy3(0, oh).start()

    def mix_loop(k):
        def body(i, c):
            mix(k, lax.rem(i + 6, 8))
            return c

        lax.fori_loop(0, 8, body, 0)
        for oh in (1, 3, 2):
            copy3(k, oh).start()

    mix_loop(2)
    mix_loop(1)
    mix_loop(3)

    h_send[...] = jnp.zeros_like(h_send)
    ones = jnp.ones((8, 128), f32)
    for k in (0, 2, 1, 3):
        for oh in (1, 3, 2):
            copy3(k, oh).wait_recv()
        block = at[THIRD[k]]
        whole = part[k, pl.ds(pl.multiple_of(block * 256, 256), 256), :]
        for i in range(3):
            whole = whole + final[k, i]
        whole = whole * whole
        sums = lax.dot_general(
            ones, whole[:, :128] + whole[:, 128:], (((1,), (1,)), ((), ())),
            preferred_element_type=f32, precision=HIGHEST,
        ) * (1.0 / (foot * probe_n))
        for i in range(2):
            h_send[pl.ds(2 * block + i, 1), :] += sums[0:1, i * 128:(i + 1) * 128]

    def first_copy(k):
        to = lax.rem(gy + k, 8)
        return pltpu.make_async_remote_copy(
            src_ref=h_send, dst_ref=h_in.at[gy],
            send_sem=h_ss.at[k], recv_sem=h_rs.at[k],
            device_id=(gx, to), device_id_type=MESH,
        )

    def second_copy(k):
        to = lax.rem(gx // 4 + k // 4, 4) * 4 + lax.rem(lax.rem(gx, 4) + k % 4, 4)
        return pltpu.make_async_remote_copy(
            src_ref=h_mid, dst_ref=h_in2.at[gx],
            send_sem=h2_ss.at[k], recv_sem=h2_rs.at[k],
            device_id=(to, gy), device_id_type=MESH,
        )

    for k in range(1, 8):
        first_copy(k).start()
    h_in[gy] = h_send[...]
    mine = owner_v[...] == me
    count = jnp.where(mine, 1.0, 0.0)
    before = jnp.where(
        lax.broadcasted_iota(jnp.int32, (128, 128), 0) < lax.broadcasted_iota(jnp.int32, (128, 128), 1),
        1.0, 0.0,
    )
    above = jnp.where(
        lax.broadcasted_iota(jnp.int32, (8, 8), 1) < lax.broadcasted_iota(jnp.int32, (8, 8), 0),
        1.0, 0.0,
    )
    in_row = jnp.dot(count, before, precision=HIGHEST, preferred_element_type=f32)
    rank = in_row + jnp.dot(
        above, jnp.broadcast_to(jnp.sum(count, axis=1, keepdims=True), (8, 128)),
        precision=HIGHEST, preferred_element_type=f32,
    )
    rank = jnp.where(mine, rank, -1.0)
    for k in range(1, 8):
        first_copy(k).wait_recv()
    total = h_in[0]
    for k in range(1, 8):
        total = total + h_in[k]
    h_mid[...] = total
    for k in range(1, 16):
        second_copy(k).start()
    h_in2[gx] = total
    for k in range(1, 16):
        second_copy(k).wait_recv()
    total = h_in2[0]
    for k in range(1, 16):
        total = total + h_in2[k]

    gain = weights_v[...] * jnp.sqrt(1.0 + total)
    new = 1024.0 * gain / jnp.sum(gain)
    new_o[...] = new
    for k in range(8):
        sens_o[k:k + 1, :] = jnp.broadcast_to(
            jnp.sum(jnp.where(rank == float(k), total, 0.0), keepdims=True), (1, 128)
        )

    ids = ids_v[...]
    lane = lax.broadcasted_iota(jnp.int32, (128, 128), 1)
    picked = jnp.zeros((128, 128), f32)
    for k in range(8):
        picked = picked + jnp.where(ids == lane + k * 128, new_o[k:k + 1, :], 0.0)
    wide[...] = jnp.broadcast_to(jnp.sum(picked, axis=1, keepdims=True), (128, 128))

    def weigh(i, acc):
        for u in range(8):
            slot = i * 8 + u
            acc = acc + wide[pl.ds(slot, 1), :] * dens[slot]
        return acc

    out = lax.fori_loop(0, 16, weigh, jnp.zeros((64, 128), f32))
    dens_o[:, :128] = out[:32]
    dens_o[:, 128:] = out[32:]

    def drain1(pos, c):
        for k in range(4):
            @pl.when(lax.rem(pos, 8) != 3)
            def _():
                copy1(k, pos).wait_send()
        return c

    def drain2(pos, c):
        for k in range(4):
            copy2(k, pos).wait_send()
        return c

    lax.fori_loop(0, 32, drain1, 0)
    lax.fori_loop(0, 24, drain2, 0)
    for k in range(4):
        for of, oc in others:
            meta1(k, of, oc).wait_send()
        for og in (1, 3, 2):
            meta2(k, og).wait_send()
            copy3(k, og).wait_send()
    for k in range(1, 8):
        first_copy(k).wait_send()
    for k in range(1, 16):
        second_copy(k).wait_send()


def local(probes, blk_rows, blk_sensor, blk_count, coef, owner, weights):
    tile_r, tile_c, probe_n = probes.shape
    nblk, foot = blk_rows.shape
    f32, bf16 = jnp.float32, jnp.bfloat16
    alive = jnp.arange(nblk, dtype=jnp.int32) < blk_count[0]
    coef_m = jnp.where(alive[:, None], coef.astype(f32), 0.0)
    rows_t = blk_rows.T.reshape(-1)
    ids = jnp.broadcast_to(blk_sensor.astype(f32)[None, :], (foot, nblk))
    meta = jnp.stack([coef_m.T, ids], axis=1)
    ids_v = jnp.broadcast_to(blk_sensor[:, None], (nblk, 128))
    vmem = pl.BlockSpec(memory_space=pltpu.VMEM)
    smem = pl.BlockSpec(memory_space=pltpu.SMEM)
    dma = pltpu.SemaphoreType.DMA
    sens, new, dens = pl.pallas_call(
        kernel,
        out_shape=(
            jax.ShapeDtypeStruct((8, 128), f32),
            jax.ShapeDtypeStruct((8, 128), f32),
            jax.ShapeDtypeStruct((tile_r, tile_c), f32),
        ),
        in_specs=[smem] + [vmem] * 7,
        out_specs=(vmem, vmem, vmem),
        scratch_shapes=[
            pltpu.VMEM((tile_r * tile_c, 2, 128), f32),
            pltpu.VMEM((3, 256, 128), f32),
            pltpu.VMEM((4, 32, nblk, probe_n), bf16),
            pltpu.VMEM((4, 7, 8, nblk, probe_n), bf16),
            pltpu.VMEM((4, 8, 8, 2, 128), f32),
            pltpu.VMEM((nblk, 64, 128), f32),
            pltpu.VMEM((4, 1024, probe_n), f32),
            pltpu.VMEM((4, 3, 256, probe_n), f32),
            pltpu.VMEM((256, 128), bf16),
            pltpu.VMEM((8, 128), f32),
            pltpu.VMEM((8, 8, 128), f32),
            pltpu.VMEM((8, 128), f32),
            pltpu.VMEM((16, 8, 128), f32),
            pltpu.VMEM((128, 128), f32),
            dma((4, 32)), dma((4, 32)), dma((4, 32)), dma((4, 32)),
            dma((4, 8)), dma((4, 8)), dma((4, 4)), dma((4, 4)),
            dma((4, 4)), dma((4, 4)),
            dma((8,)), dma((8,)), dma((16,)), dma((16,)),
        ],
        compiler_params=pltpu.CompilerParams(
            collective_id=0, has_side_effects=True, vmem_limit_bytes=60 * 2 ** 20
        ),
        name="exchange",
    )(
        rows_t, probes.reshape(tile_r * tile_c, probe_n), meta, blk_rows, coef_m, ids_v,
        owner.reshape(8, 128), weights.reshape(8, 128),
    )
    return sens[:, 0], new.reshape(-1), dens


def solution(mesh):
    in_specs = (
        P("gx", "gy", None),
        P(("gx", "gy"), None),
        P(("gx", "gy")),
        P(("gx", "gy")),
        P(("gx", "gy"), None),
        P(),
        P(),
    )
    out_specs = (P(("gx", "gy")), P(), P("gx", "gy"))
    return jax.shard_map(local, mesh=mesh, in_specs=in_specs, out_specs=out_specs, check_vma=False)
```

```python
import jax
import jax.numpy as jnp
from jax import lax
from jax.experimental import pallas as pl
from jax.experimental.pallas import tpu as pltpu
from jax.sharding import PartitionSpec as P

MESH = pl.DeviceIdType.MESH
HIGHEST = lax.Precision.HIGHEST
FIRST = (0, 1, 2, 2)
SECOND = (1, 2, 0, 0)
THIRD = (2, 0, 1, 1)


def place():
    gx, gy = lax.axis_index("gx"), lax.axis_index("gy")
    return [lax.rem(gx, 4), gx // 4, gy // 2], lax.rem(gy, 2)


def peer(axis, off, core_off):
    at, core = place()
    at[axis] = lax.rem(at[axis] + off, 4)
    return at[1] * 4 + at[0], at[2] * 2 + lax.rem(core + core_off, 2)


def order(i):
    return lax.rem(1 + 2 * i - 3 * (i // 2), 4)


def decode(pos):
    return order(pos // 8), order(lax.rem(pos, 4)), lax.rem(pos, 8) // 4


def kernel(
    rows_s, count_v, probes_h, rows_v, coef_b, ids_r, owner_v, weights_v,
    sens_o, new_o, dens_o,
    probes, tile, stage, send, zone, meta, metas, coef_v, ids_v, dens, part, final, steps_v,
    h_send, h_in, h_mid, h_in2, wide,
    in_sem, sent, rs1, rs2, m_sem, fr, h_sem,
):
    n_pts, probe_n = probes.shape
    foot = 128
    chunk = n_pts // 4
    gx, gy = lax.axis_index("gx"), lax.axis_index("gy")
    me = gx * 8 + gy
    at, core = place()
    bf16, f32 = jnp.bfloat16, jnp.float32

    def load(i):
        part_of = pl.ds(i * chunk, chunk)
        return pltpu.make_async_copy(probes_h.at[part_of], probes.at[part_of], in_sem.at[i])

    for i in range(4):
        load(i).start()
    barrier = pltpu.get_barrier_semaphore()

    def greet(device):
        pl.semaphore_signal(barrier, inc=1, device_id=device, device_id_type=MESH)

    for k in range(1, 16):
        greet((lax.rem(gx // 4 + k // 4, 4) * 4 + lax.rem(lax.rem(gx, 4) + k % 4, 4), gy))
    for k in range(1, 8):
        greet((gx, lax.rem(gy + k, 8)))
    for axis in (0, 1):
        for off in (1, 2, 3):
            greet(peer(axis, off, 1))

    flat = tile.reshape(2 * n_pts, 128)

    def widen(i, c):
        block = probes[pl.ds(pl.multiple_of(i * 64, 64), 64), :].astype(f32)
        flat[pl.ds(i * 128, 64, 2), :] = block[:, :128]
        flat[pl.ds(i * 128 + 1, 64, 2), :] = block[:, 128:]
        return c

    slot_of = lax.broadcasted_iota(jnp.int32, (128, 128), 0)
    coef_v[...] = jnp.where(slot_of < count_v[...], coef_b[...].astype(f32), 0.0)
    names_r = jnp.broadcast_to(ids_r[...].astype(f32), (128, 128))
    meta[:, 0, :] = coef_v[...].T
    meta[:, 1, :] = names_r
    ids_v[...] = names_r.T
    for i in range(4):
        load(i).wait()
        lax.fori_loop(i * (chunk // 64), (i + 1) * (chunk // 64), widen, 0)
    for i in range(16):
        steps_v[i * 16:(i + 1) * 16, :] = (
            lax.broadcasted_iota(jnp.int32, (16, 128), 0) + i * 16
        ).astype(f32).astype(bf16)

    def meta1(k, of, oc):
        first = lax.rem(core + oc, 2) * 64 + k * 16 + lax.rem(at[FIRST[k]] + of, 4) * 4
        src = oc * 4 + of
        return pltpu.make_async_remote_copy(
            src_ref=meta.at[pl.ds(first, 4)], dst_ref=metas.at[k, pl.ds(0, 4), src],
            send_sem=m_sem.at[0, k], recv_sem=m_sem.at[1, k],
            device_id=peer(FIRST[k], of, oc), device_id_type=MESH,
        )

    def meta2(k, og):
        return pltpu.make_async_remote_copy(
            src_ref=metas.at[k, lax.rem(at[SECOND[k]] + og, 4)], dst_ref=metas.at[k, 4 + og],
            send_sem=m_sem.at[2, k], recv_sem=m_sem.at[3, k],
            device_id=peer(SECOND[k], og, 0), device_id_type=MESH,
        )

    def copy1(k, pos):
        og, of, oc = decode(pos)
        return pltpu.make_async_remote_copy(
            src_ref=send.at[k, pos], dst_ref=zone.at[k, og + 3 * ((og + 3) // 4), oc * 4 + of],
            send_sem=sent.at[0, k], recv_sem=rs1.at[k, pos // 4],
            device_id=peer(FIRST[k], of, oc), device_id_type=MESH,
        )

    def copy2(k, og, oc):
        return pltpu.make_async_remote_copy(
            src_ref=zone.at[k, 3 + og, oc * 4:oc * 4 + 4], dst_ref=zone.at[k, og, oc * 4:oc * 4 + 4],
            send_sem=sent.at[1, k], recv_sem=rs2.at[k, og * 2 + oc],
            device_id=peer(SECOND[k], og, 0), device_id_type=MESH,
        )

    def await_bytes(ref, sem):
        pltpu.make_async_copy(ref, ref, sem).wait()

    def copy3(k, oh):
        block = lax.rem(at[THIRD[k]] + oh, 4)
        return pltpu.make_async_remote_copy(
            src_ref=part.at[k, pl.ds(pl.multiple_of(block * 256, 256), 256)], dst_ref=final.at[k, oh - 1],
            send_sem=sent.at[2, k], recv_sem=fr.at[k],
            device_id=peer(THIRD[k], oh, 0), device_id_type=MESH,
        )

    others = [(of, oc) for oc in (0, 1) for of in (1, 3, 2, 0) if (of, oc) != (0, 0)]
    for k in range(4):
        metas[k, 0:4, 0] = meta[pl.ds(core * 64 + k * 16 + at[FIRST[k]] * 4, 4)]

    def gather(k, pos, buf):
        og, of, oc = decode(pos)
        chan = (
            lax.rem(core + oc, 2) * 64 + k * 16
            + lax.rem(at[FIRST[k]] + of, 4) * 4 + lax.rem(at[SECOND[k]] + og, 4)
        )
        for i in range(128):
            stage[buf, 2 * i:2 * i + 2, :] = tile[rows_s[chan + i * 128]]
        send[k, pos, :, :128] = stage[buf, pl.ds(0, 128, 2), :].astype(bf16)
        send[k, pos, :, 128:] = stage[buf, pl.ds(1, 128, 2), :].astype(bf16)

    def give(k, pos):
        mine = lax.rem(pos, 8) == 3

        @pl.when(mine)
        def _():
            og, _, _ = decode(pos)
            zone[k, og + 3 * ((og + 3) // 4), 0] = send[k, pos]

        @pl.when(jnp.logical_not(mine))
        def _():
            copy1(k, pos).start()

    def first_loop(pos, c):
        for buf, k in enumerate((2, 0, 1)):
            gather(k, pos, buf)
            if buf == 0:
                @pl.when(pos == 1)
                def _():
                    pl.semaphore_wait(barrier, 28)

            @pl.when(pos > 0)
            def _():
                give(k, pos - 1)

        @pl.when(pos == 2)
        def _():
            for of, oc in others:
                for k in range(4):
                    meta1(k, of, oc).start()
        return c

    lax.fori_loop(0, 32, first_loop, 0)

    def second_loop(pos, c):
        gather(3, pos, 0)

        @pl.when(pos == 0)
        def _():
            for k in (2, 0, 1):
                give(k, 31)

        @pl.when(pos > 0)
        def _():
            give(3, pos - 1)
        return c

    def forward(k, i):
        og = order(i)
        for oc in (0, 1):
            await_bytes(zone.at[k, 3 + og, (1 if oc == 0 else 4):oc * 4 + 4], rs1.at[k, 2 * i + oc])
            copy2(k, og, oc).start()

    forward(2, 0)
    lax.fori_loop(0, 32, second_loop, 0)
    give(3, 31)

    for k in range(4):
        await_bytes(metas.at[k, 0:4, 1:8], m_sem.at[1, k])
    for og in (1, 3, 2):
        for k in range(4):
            meta2(k, og).start()

    q = lax.broadcasted_iota(jnp.int32, (64, 128), 0)
    hi_of = jnp.where(q < 32, 2 * q, 2 * q - 63)
    lo_of = lax.broadcasted_iota(jnp.int32, (128, 128), 0)

    def spread(first):
        for u in range(4):
            row = rows_v[pl.ds(first + u, 1), :]
            val = coef_v[pl.ds(first + u, 1), :]
            high = jnp.where(row // 128 == hi_of, val, 0.0).astype(bf16)
            low = jnp.where(lax.rem(row, 128) == lo_of, val, 0.0).astype(bf16)
            dens[first + u] = lax.dot_general(
                high, low, (((1,), (1,)), ((), ())), preferred_element_type=f32
            )

    def spread_loop(i, c):
        spread(i * 4)
        return c

    forward(2, 1)
    forward(0, 0)
    forward(1, 0)
    lax.fori_loop(0, 12, spread_loop, 0)
    for k in (0, 2, 1):
        if k != 2:
            forward(k, 1)
        forward(k, 2)
    lax.fori_loop(12, 24, spread_loop, 0)
    part[...] = jnp.zeros_like(part)

    def mix(k, group):
        og, oc = order(group // 2), lax.rem(group, 2)

        @pl.when(group < 6)
        def _():
            await_bytes(zone.at[k, og, pl.ds(oc * 4, 4)], rs2.at[k, og * 2 + oc])

        @pl.when(group == 6)
        def _():
            await_bytes(zone.at[k, 0, 1:4], rs1.at[k, 6])

        @pl.when(group == 7)
        def _():
            await_bytes(zone.at[k, 0, 4:8], rs1.at[k, 7])

        cols = zone[k, og, pl.ds(oc * 4, 4)].reshape(512, probe_n)
        slot = og + 4 * ((og + 3) // 4) + at[SECOND[k]] * (1 - (og + 3) // 4)
        tags = [metas[k, slot, oc * 4 + u] for u in range(4)]
        vals = [jnp.broadcast_to(t[0:1], (16, 128)).astype(bf16) for t in tags]
        zero = jnp.zeros((16, 128), bf16)
        for m in range(4):
            names = [jnp.broadcast_to(t[1:2] - float(m * 256), (16, 128)).astype(bf16) for t in tags]
            mixer = jnp.concatenate(
                [
                    jnp.concatenate(
                        [
                            jnp.where(names[u] == steps_v[i * 16:(i + 1) * 16, :], vals[u], zero)
                            for i in range(16)
                        ],
                        axis=0,
                    )
                    for u in range(4)
                ],
                axis=1,
            )
            part[k, m * 256:(m + 1) * 256, :] += jnp.dot(mixer, cols, preferred_element_type=f32)

    for k in range(4):
        await_bytes(metas.at[k, 5:8], m_sem.at[3, k])
    for i in range(3):
        spread(96 + i * 8)
        spread(100 + i * 8)
        mix(0, 6 + i if i < 2 else 0)
        forward(3, i)
    spread(120)
    spread(124)

    def mix_loop(*kinds):
        def body(i, c):
            for k in kinds:
                mix(k, lax.rem(i + 6, 8))
            return c
        return body

    lax.fori_loop(3, 8, mix_loop(0), 0)
    for oh in (1, 3, 2):
        copy3(0, oh).start()
    lax.fori_loop(0, 8, mix_loop(2), 0)
    for oh in (1, 3, 2):
        copy3(2, oh).start()
    lax.fori_loop(0, 8, mix_loop(1, 3), 0)
    for k in (1, 3):
        for oh in (1, 3, 2):
            copy3(k, oh).start()

    h_send[...] = jnp.zeros_like(h_send)
    ones = jnp.ones((8, 128), f32)
    for k in (0, 2, 1, 3):
        await_bytes(final.at[k], fr.at[k])
        block = at[THIRD[k]]
        whole = part[k, pl.ds(pl.multiple_of(block * 256, 256), 256), :]
        for i in range(3):
            whole = whole + final[k, i]
        whole = whole * whole
        sums = lax.dot_general(
            ones, whole[:, :128] + whole[:, 128:], (((1,), (1,)), ((), ())),
            preferred_element_type=f32, precision=HIGHEST,
        ) * (1.0 / (foot * probe_n))
        for i in range(2):
            h_send[pl.ds(2 * block + i, 1), :] += sums[0:1, i * 128:(i + 1) * 128]

    def first_copy(k):
        to = lax.rem(gy + k, 8)
        return pltpu.make_async_remote_copy(
            src_ref=h_send, dst_ref=h_in.at[gy],
            send_sem=h_sem.at[0], recv_sem=h_sem.at[1],
            device_id=(gx, to), device_id_type=MESH,
        )

    def second_copy(k):
        to = lax.rem(gx // 4 + k // 4, 4) * 4 + lax.rem(lax.rem(gx, 4) + k % 4, 4)
        return pltpu.make_async_remote_copy(
            src_ref=h_mid, dst_ref=h_in2.at[gx],
            send_sem=h_sem.at[2], recv_sem=h_sem.at[3],
            device_id=(to, gy), device_id_type=MESH,
        )

    for k in range(1, 8):
        first_copy(k).start()
    h_in[gy] = h_send[...]
    mine = owner_v[...] == me
    count = jnp.where(mine, 1.0, 0.0)
    before = jnp.where(
        lax.broadcasted_iota(jnp.int32, (128, 128), 0) < lax.broadcasted_iota(jnp.int32, (128, 128), 1),
        1.0, 0.0,
    )
    above = jnp.where(
        lax.broadcasted_iota(jnp.int32, (8, 8), 1) < lax.broadcasted_iota(jnp.int32, (8, 8), 0),
        1.0, 0.0,
    )
    in_row = jnp.dot(count, before, precision=HIGHEST, preferred_element_type=f32)
    rank = in_row + jnp.dot(
        above, jnp.broadcast_to(jnp.sum(count, axis=1, keepdims=True), (8, 128)),
        precision=HIGHEST, preferred_element_type=f32,
    )
    rank = jnp.where(mine, rank, -1.0)
    await_bytes(h_in.at[1:8], h_sem.at[1])
    total = h_in[0]
    for k in range(1, 8):
        total = total + h_in[k]
    h_mid[...] = total
    for k in range(1, 16):
        second_copy(k).start()
    h_in2[gx] = total
    await_bytes(h_in2.at[1:16], h_sem.at[3])
    total = h_in2[0]
    for k in range(1, 16):
        total = total + h_in2[k]

    gain = weights_v[...] * jnp.sqrt(1.0 + total)
    new = 1024.0 * gain / jnp.sum(gain)
    new_o[...] = new
    for k in range(8):
        sens_o[k] = jnp.sum(jnp.where(rank == float(k), total, 0.0))

    ids = ids_v[...]
    lane = lax.broadcasted_iota(jnp.int32, (128, 128), 1)
    picked = jnp.zeros((128, 128), f32)
    for k in range(8):
        picked = picked + jnp.where(ids == (lane + k * 128).astype(f32), new_o[k:k + 1, :], 0.0)
    wide[...] = jnp.broadcast_to(jnp.sum(picked, axis=1, keepdims=True), (128, 128))

    def weigh(i, acc):
        for u in range(8):
            slot = i * 8 + u
            acc = acc + wide[pl.ds(slot, 1), :] * dens[slot]
        return acc

    out = lax.fori_loop(0, 16, weigh, jnp.zeros((64, 128), f32))
    dens_o[:, :128] = out[:32]
    dens_o[:, 128:] = out[32:]

    for k in range(4):
        await_bytes(send.at[k, 0:28], sent.at[0, k])
        await_bytes(zone.at[k, 1:4], sent.at[1, k])
        await_bytes(final.at[k], sent.at[2, k])
        await_bytes(metas.at[k, 0:4, 1:8], m_sem.at[0, k])
        await_bytes(metas.at[k, 5:8], m_sem.at[2, k])
    await_bytes(h_in.at[1:8], h_sem.at[0])
    await_bytes(h_in2.at[1:16], h_sem.at[2])


def finish(sens, new, dens, sens_o, new_o, dens_o):
    for k in range(8):
        sens_o[k] = sens[k]
    new_o[...] = new[...]
    dens_o[...] = dens[...]


def local(probes, blk_rows, blk_sensor, blk_count, coef, owner, weights):
    tile_r, tile_c, probe_n = probes.shape
    nblk, foot = blk_rows.shape
    f32, bf16 = jnp.float32, jnp.bfloat16
    vmem = pl.BlockSpec(memory_space=pltpu.VMEM)
    smem = pl.BlockSpec(memory_space=pltpu.SMEM)
    anyw = pl.BlockSpec(memory_space=pl.ANY)
    dma = pltpu.SemaphoreType.DMA
    outs = (
        jax.ShapeDtypeStruct((8,), f32),
        jax.ShapeDtypeStruct((8, 128), f32),
        jax.ShapeDtypeStruct((tile_r, tile_c), f32),
    )
    sens, new, dens = pl.pallas_call(
        kernel,
        out_shape=outs,
        in_specs=[smem, vmem, anyw] + [vmem] * 5,
        out_specs=(smem, vmem, vmem),
        scratch_shapes=[
            pltpu.VMEM((tile_r * tile_c, probe_n), bf16),
            pltpu.VMEM((tile_r * tile_c, 2, 128), f32),
            pltpu.VMEM((3, 256, 128), f32),
            pltpu.VMEM((4, 32, nblk, probe_n), bf16),
            pltpu.VMEM((4, 7, 8, nblk, probe_n), bf16),
            pltpu.VMEM((128, 2, 128), f32),
            pltpu.VMEM((4, 8, 8, 2, 128), f32),
            pltpu.VMEM((nblk, foot), f32),
            pltpu.VMEM((nblk, foot), f32),
            pltpu.VMEM((nblk, 64, 128), f32),
            pltpu.VMEM((4, 1024, probe_n), f32),
            pltpu.VMEM((4, 3, 256, probe_n), f32),
            pltpu.VMEM((256, 128), bf16),
            pltpu.VMEM((8, 128), f32),
            pltpu.VMEM((8, 8, 128), f32),
            pltpu.VMEM((8, 128), f32),
            pltpu.VMEM((16, 8, 128), f32),
            pltpu.VMEM((128, 128), f32),
            dma((4,)), dma((3, 4)), dma((4, 8)), dma((4, 8)), dma((4, 4)), dma((4,)), dma((4,)),
        ],
        compiler_params=pltpu.CompilerParams(
            collective_id=0, has_side_effects=True, vmem_limit_bytes=60 * 2 ** 20
        ),
        name="exchange",
    )(
        blk_rows.reshape(-1), blk_count.reshape(1, 1), probes.reshape(tile_r * tile_c, probe_n), blk_rows, coef,
        blk_sensor.reshape(1, nblk), owner.reshape(8, 128), weights.reshape(8, 128),
    )
    sens, new, dens = pl.pallas_call(
        finish, out_shape=outs, in_specs=[smem, vmem, vmem], out_specs=(smem, vmem, vmem), name="finish",
    )(sens, new, dens)
    return sens, new.reshape(-1), dens


def solution(mesh):
    in_specs = (
        P("gx", "gy", None),
        P(("gx", "gy"), None),
        P(("gx", "gy")),
        P(("gx", "gy")),
        P(("gx", "gy"), None),
        P(),
        P(),
    )
    out_specs = (P(("gx", "gy")), P(), P("gx", "gy"))
    return jax.shard_map(local, mesh=mesh, in_specs=in_specs, out_specs=out_specs, check_vma=False)
```

```python
import jax
import jax.numpy as jnp
from jax import lax
from jax.experimental import pallas as pl
from jax.experimental.pallas import tpu as pltpu
from jax.sharding import PartitionSpec as P

MESH = pl.DeviceIdType.MESH
HIGHEST = lax.Precision.HIGHEST
FIRST = (0, 1, 2, 2)
SECOND = (1, 2, 0, 0)
THIRD = (2, 0, 1, 1)


def place():
    gx, gy = lax.axis_index("gx"), lax.axis_index("gy")
    return [lax.rem(gx, 4), gx // 4, gy // 2], lax.rem(gy, 2)


def peer(axis, off, core_off):
    at, core = place()
    at[axis] = lax.rem(at[axis] + off, 4)
    return at[1] * 4 + at[0], at[2] * 2 + lax.rem(core + core_off, 2)


def order(i):
    return lax.rem(1 + 2 * i - 3 * (i // 2), 4)


def decode(pos):
    return order(pos // 8), order(lax.rem(pos, 4)), lax.rem(pos, 8) // 4


def kernel(
    rows_h, count_v, probes_h, rows_v, coef_b, ids_r, owner_v, weights_v,
    sens_o, new_o, dens_o,
    rows_s, probes, tile, stage, send, zone, meta, metas, coef_v, ids_v, dens, part, final, steps_v,
    h_send, h_in, h_mid, h_in2, wide,
    in_sem, row_sem, sent, rs1, rs2, m_sem, fr, h_sem,
):
    n_pts, probe_n = probes.shape
    foot = 128
    chunk = n_pts // 4
    gx, gy = lax.axis_index("gx"), lax.axis_index("gy")
    me = gx * 8 + gy
    at, core = place()
    bf16, f32 = jnp.bfloat16, jnp.float32

    def load(i):
        part_of = pl.ds(i * chunk, chunk)
        return pltpu.make_async_copy(probes_h.at[part_of], probes.at[part_of], in_sem.at[i])

    rows_in = pltpu.make_async_copy(rows_h, rows_s, row_sem)
    for i in range(4):
        load(i).start()
    rows_in.start()
    barrier = pltpu.get_barrier_semaphore()

    def greet(device):
        pl.semaphore_signal(barrier, inc=1, device_id=device, device_id_type=MESH)

    for k in range(1, 16):
        greet((lax.rem(gx // 4 + k // 4, 4) * 4 + lax.rem(lax.rem(gx, 4) + k % 4, 4), gy))
    for k in range(1, 8):
        greet((gx, lax.rem(gy + k, 8)))
    for axis in (0, 1):
        for off in (1, 2, 3):
            greet(peer(axis, off, 1))

    flat = tile.reshape(2 * n_pts, 128)

    def widen(i, c):
        block = probes[pl.ds(pl.multiple_of(i * 64, 64), 64), :].astype(f32)
        flat[pl.ds(i * 128, 64, 2), :] = block[:, :128]
        flat[pl.ds(i * 128 + 1, 64, 2), :] = block[:, 128:]
        return c

    slot_of = lax.broadcasted_iota(jnp.int32, (128, 128), 0)
    coef_v[...] = jnp.where(slot_of < count_v[...], coef_b[...].astype(f32), 0.0)
    names_r = jnp.broadcast_to(ids_r[...].astype(f32), (128, 128))
    meta[:, 0, :] = coef_v[...].T
    meta[:, 1, :] = names_r
    ids_v[...] = names_r.T
    for i in range(4):
        load(i).wait()
        lax.fori_loop(i * (chunk // 64), (i + 1) * (chunk // 64), widen, 0)
    rows_in.wait()
    for i in range(16):
        steps_v[i * 16:(i + 1) * 16, :] = (
            lax.broadcasted_iota(jnp.int32, (16, 128), 0) + i * 16
        ).astype(f32).astype(bf16)

    def meta1(k, of, oc):
        first = lax.rem(core + oc, 2) * 64 + k * 16 + lax.rem(at[FIRST[k]] + of, 4) * 4
        src = oc * 4 + of
        return pltpu.make_async_remote_copy(
            src_ref=meta.at[pl.ds(first, 4)], dst_ref=metas.at[k, pl.ds(0, 4), src],
            send_sem=m_sem.at[0, k], recv_sem=m_sem.at[1, k],
            device_id=peer(FIRST[k], of, oc), device_id_type=MESH,
        )

    def meta2(k, og):
        return pltpu.make_async_remote_copy(
            src_ref=metas.at[k, lax.rem(at[SECOND[k]] + og, 4)], dst_ref=metas.at[k, 4 + og],
            send_sem=m_sem.at[2, k], recv_sem=m_sem.at[3, k],
            device_id=peer(SECOND[k], og, 0), device_id_type=MESH,
        )

    def copy1(k, pos):
        og, of, oc = decode(pos)
        return pltpu.make_async_remote_copy(
            src_ref=send.at[k, pos], dst_ref=zone.at[k, og + 3 * ((og + 3) // 4), oc * 4 + of],
            send_sem=sent.at[0, k], recv_sem=rs1.at[k, pos // 4],
            device_id=peer(FIRST[k], of, oc), device_id_type=MESH,
        )

    def copy2(k, og, oc):
        return pltpu.make_async_remote_copy(
            src_ref=zone.at[k, 3 + og, oc * 4:oc * 4 + 4], dst_ref=zone.at[k, og, oc * 4:oc * 4 + 4],
            send_sem=sent.at[1, k], recv_sem=rs2.at[k, og * 2 + oc],
            device_id=peer(SECOND[k], og, 0), device_id_type=MESH,
        )

    def await_bytes(ref, sem):
        pltpu.make_async_copy(ref, ref, sem).wait()

    def copy3(k, oh):
        block = lax.rem(at[THIRD[k]] + oh, 4)
        return pltpu.make_async_remote_copy(
            src_ref=part.at[k, pl.ds(pl.multiple_of(block * 256, 256), 256)], dst_ref=final.at[k, oh - 1],
            send_sem=sent.at[2, k], recv_sem=fr.at[k],
            device_id=peer(THIRD[k], oh, 0), device_id_type=MESH,
        )

    others = [(of, oc) for oc in (0, 1) for of in (1, 3, 2, 0) if (of, oc) != (0, 0)]
    for k in range(4):
        metas[k, 0:4, 0] = meta[pl.ds(core * 64 + k * 16 + at[FIRST[k]] * 4, 4)]

    def gather(k, pos, buf):
        og, of, oc = decode(pos)
        chan = (
            lax.rem(core + oc, 2) * 64 + k * 16
            + lax.rem(at[FIRST[k]] + of, 4) * 4 + lax.rem(at[SECOND[k]] + og, 4)
        )
        for i in range(128):
            stage[buf, 2 * i:2 * i + 2, :] = tile[rows_s[chan + i * 128]]
        send[k, pos, :, :128] = stage[buf, pl.ds(0, 128, 2), :].astype(bf16)
        send[k, pos, :, 128:] = stage[buf, pl.ds(1, 128, 2), :].astype(bf16)

    def give(k, pos):
        mine = lax.rem(pos, 8) == 3

        @pl.when(mine)
        def _():
            og, _, _ = decode(pos)
            zone[k, og + 3 * ((og + 3) // 4), 0] = send[k, pos]

        @pl.when(jnp.logical_not(mine))
        def _():
            copy1(k, pos).start()

    def forward(k, i):
        og = order(i)
        for oc in (0, 1):
            await_bytes(zone.at[k, 3 + og, (1 if oc == 0 else 4):oc * 4 + 4], rs1.at[k, 2 * i + oc])
            copy2(k, og, oc).start()

    def first_loop(pos, c):
        for buf, k in enumerate((2, 0)):
            gather(k, pos, buf)
            if buf == 0:
                @pl.when(pos == 1)
                def _():
                    pl.semaphore_wait(barrier, 28)
                    for of, oc in others:
                        for j in range(4):
                            meta1(j, of, oc).start()

                @pl.when(pos == 16)
                def _():
                    for j in range(4):
                        await_bytes(metas.at[j, 0:4, 1:8], m_sem.at[1, j])
                    for og in (1, 3, 2):
                        for j in range(4):
                            meta2(j, og).start()

            @pl.when(pos > 0)
            def _():
                give(k, pos - 1)

        return c

    def second_loop(pos, c):
        for buf, k in enumerate((3, 1)):
            gather(k, pos, buf)
            if buf == 0:
                @pl.when(pos == 0)
                def _():
                    for j in (2, 0):
                        give(j, 31)

                @pl.when(pos == 16)
                def _():
                    forward(2, 1)

            @pl.when(pos > 0)
            def _():
                give(k, pos - 1)

        return c

    lax.fori_loop(0, 32, first_loop, 0)
    forward(2, 0)
    lax.fori_loop(0, 32, second_loop, 0)
    give(3, 31)
    give(1, 31)

    q = lax.broadcasted_iota(jnp.int32, (64, 128), 0)
    hi_of = jnp.where(q < 32, 2 * q, 2 * q - 63)
    lo_of = lax.broadcasted_iota(jnp.int32, (128, 128), 0)

    def spread(first):
        for u in range(4):
            row = rows_v[pl.ds(first + u, 1), :]
            val = coef_v[pl.ds(first + u, 1), :]
            high = jnp.where(row // 128 == hi_of, val, 0.0).astype(bf16)
            low = jnp.where(lax.rem(row, 128) == lo_of, val, 0.0).astype(bf16)
            dens[first + u] = lax.dot_general(
                high, low, (((1,), (1,)), ((), ())), preferred_element_type=f32
            )

    def spread_loop(i, c):
        spread(i * 4)
        return c

    def mix(k, group):
        og, oc = order(group // 2), lax.rem(group, 2)

        @pl.when(group < 6)
        def _():
            await_bytes(zone.at[k, og, pl.ds(oc * 4, 4)], rs2.at[k, og * 2 + oc])

        @pl.when(group == 6)
        def _():
            await_bytes(zone.at[k, 0, 1:4], rs1.at[k, 6])

        @pl.when(group == 7)
        def _():
            await_bytes(zone.at[k, 0, 4:8], rs1.at[k, 7])

        cols = zone[k, og, pl.ds(oc * 4, 4)].reshape(512, probe_n)
        slot = og + 4 * ((og + 3) // 4) + at[SECOND[k]] * (1 - (og + 3) // 4)
        tags = [metas[k, slot, oc * 4 + u] for u in range(4)]
        vals = [jnp.broadcast_to(t[0:1], (16, 128)).astype(bf16) for t in tags]
        zero = jnp.zeros((16, 128), bf16)
        for m in range(4):
            names = [jnp.broadcast_to(t[1:2] - float(m * 256), (16, 128)).astype(bf16) for t in tags]
            mixer = jnp.concatenate(
                [
                    jnp.concatenate(
                        [
                            jnp.where(names[u] == steps_v[i * 16:(i + 1) * 16, :], vals[u], zero)
                            for i in range(16)
                        ],
                        axis=0,
                    )
                    for u in range(4)
                ],
                axis=1,
            )
            part[k, m * 256:(m + 1) * 256, :] += jnp.dot(mixer, cols, preferred_element_type=f32)

    def mix_loop(*kinds):
        def body(i, c):
            for k in kinds:
                mix(k, lax.rem(i + 6, 8))
            return c
        return body

    def sum_up(k):
        for oh in (1, 3, 2):
            copy3(k, oh).start()

    forward(2, 2)
    for i in range(3):
        forward(0, i)
    forward(1, 0)
    part[...] = jnp.zeros_like(part)
    for k in range(4):
        await_bytes(metas.at[k, 5:8], m_sem.at[3, k])
    lax.fori_loop(0, 16, spread_loop, 0)
    forward(3, 0)
    forward(1, 1)
    lax.fori_loop(16, 32, spread_loop, 0)
    lax.fori_loop(0, 4, mix_loop(2), 0)
    forward(1, 2)
    forward(3, 1)
    lax.fori_loop(4, 8, mix_loop(2), 0)
    sum_up(2)
    lax.fori_loop(0, 4, mix_loop(0), 0)
    forward(3, 2)
    lax.fori_loop(4, 8, mix_loop(0), 0)
    sum_up(0)
    lax.fori_loop(0, 8, mix_loop(1, 3), 0)
    sum_up(1)
    sum_up(3)

    h_send[...] = jnp.zeros_like(h_send)
    ones = jnp.ones((8, 128), f32)
    for k in (2, 0, 1, 3):
        await_bytes(final.at[k], fr.at[k])
        block = at[THIRD[k]]
        whole = part[k, pl.ds(pl.multiple_of(block * 256, 256), 256), :]
        for i in range(3):
            whole = whole + final[k, i]
        whole = whole * whole
        sums = lax.dot_general(
            ones, whole[:, :128] + whole[:, 128:], (((1,), (1,)), ((), ())),
            preferred_element_type=f32, precision=HIGHEST,
        ) * (1.0 / (foot * probe_n))
        for i in range(2):
            h_send[pl.ds(2 * block + i, 1), :] += sums[0:1, i * 128:(i + 1) * 128]

    def first_copy(k):
        to = lax.rem(gy + k, 8)
        return pltpu.make_async_remote_copy(
            src_ref=h_send, dst_ref=h_in.at[gy],
            send_sem=h_sem.at[0], recv_sem=h_sem.at[1],
            device_id=(gx, to), device_id_type=MESH,
        )

    def second_copy(k):
        to = lax.rem(gx // 4 + k // 4, 4) * 4 + lax.rem(lax.rem(gx, 4) + k % 4, 4)
        return pltpu.make_async_remote_copy(
            src_ref=h_mid, dst_ref=h_in2.at[gx],
            send_sem=h_sem.at[2], recv_sem=h_sem.at[3],
            device_id=(to, gy), device_id_type=MESH,
        )

    for k in range(1, 8):
        first_copy(k).start()
    h_in[gy] = h_send[...]
    mine = owner_v[...] == me
    count = jnp.where(mine, 1.0, 0.0)
    before = jnp.where(
        lax.broadcasted_iota(jnp.int32, (128, 128), 0) < lax.broadcasted_iota(jnp.int32, (128, 128), 1),
        1.0, 0.0,
    )
    above = jnp.where(
        lax.broadcasted_iota(jnp.int32, (8, 8), 1) < lax.broadcasted_iota(jnp.int32, (8, 8), 0),
        1.0, 0.0,
    )
    in_row = jnp.dot(count, before, precision=HIGHEST, preferred_element_type=f32)
    rank = in_row + jnp.dot(
        above, jnp.broadcast_to(jnp.sum(count, axis=1, keepdims=True), (8, 128)),
        precision=HIGHEST, preferred_element_type=f32,
    )
    rank = jnp.where(mine, rank, -1.0)
    await_bytes(h_in.at[1:8], h_sem.at[1])
    total = h_in[0]
    for k in range(1, 8):
        total = total + h_in[k]
    h_mid[...] = total
    for k in range(1, 16):
        second_copy(k).start()
    h_in2[gx] = total
    await_bytes(h_in2.at[1:16], h_sem.at[3])
    total = h_in2[0]
    for k in range(1, 16):
        total = total + h_in2[k]

    gain = weights_v[...] * jnp.sqrt(1.0 + total)
    new = 1024.0 * gain / jnp.sum(gain)
    new_o[...] = new
    for k in range(8):
        sens_o[k] = jnp.sum(jnp.where(rank == float(k), total, 0.0))

    ids = ids_v[...]
    lane = lax.broadcasted_iota(jnp.int32, (128, 128), 1)
    picked = jnp.zeros((128, 128), f32)
    for k in range(8):
        picked = picked + jnp.where(ids == (lane + k * 128).astype(f32), new_o[k:k + 1, :], 0.0)
    wide[...] = jnp.broadcast_to(jnp.sum(picked, axis=1, keepdims=True), (128, 128))

    def weigh(i, acc):
        for u in range(8):
            slot = i * 8 + u
            acc = acc + wide[pl.ds(slot, 1), :] * dens[slot]
        return acc

    out = lax.fori_loop(0, 16, weigh, jnp.zeros((64, 128), f32))
    dens_o[:, :128] = out[:32]
    dens_o[:, 128:] = out[32:]

    for k in range(4):
        await_bytes(send.at[k, 0:28], sent.at[0, k])
        await_bytes(zone.at[k, 1:4], sent.at[1, k])
        await_bytes(final.at[k], sent.at[2, k])
        await_bytes(metas.at[k, 0:4, 1:8], m_sem.at[0, k])
        await_bytes(metas.at[k, 5:8], m_sem.at[2, k])
    await_bytes(h_in.at[1:8], h_sem.at[0])
    await_bytes(h_in2.at[1:16], h_sem.at[2])


def finish(sens, new, dens, sens_o, new_o, dens_o):
    for k in range(8):
        sens_o[k] = sens[k]
    new_o[...] = new[...]
    dens_o[...] = dens[...]


def local(probes, blk_rows, blk_sensor, blk_count, coef, owner, weights):
    tile_r, tile_c, probe_n = probes.shape
    nblk, foot = blk_rows.shape
    f32, bf16 = jnp.float32, jnp.bfloat16
    vmem = pl.BlockSpec(memory_space=pltpu.VMEM)
    smem = pl.BlockSpec(memory_space=pltpu.SMEM)
    anyw = pl.BlockSpec(memory_space=pl.ANY)
    dma = pltpu.SemaphoreType.DMA
    outs = (
        jax.ShapeDtypeStruct((8,), f32),
        jax.ShapeDtypeStruct((8, 128), f32),
        jax.ShapeDtypeStruct((tile_r, tile_c), f32),
    )
    sens, new, dens = pl.pallas_call(
        kernel,
        out_shape=outs,
        in_specs=[anyw, vmem, anyw] + [vmem] * 5,
        out_specs=(smem, vmem, vmem),
        scratch_shapes=[
            pltpu.SMEM((nblk * foot,), jnp.int32),
            pltpu.VMEM((tile_r * tile_c, probe_n), bf16),
            pltpu.VMEM((tile_r * tile_c, 2, 128), f32),
            pltpu.VMEM((3, 256, 128), f32),
            pltpu.VMEM((4, 32, nblk, probe_n), bf16),
            pltpu.VMEM((4, 7, 8, nblk, probe_n), bf16),
            pltpu.VMEM((128, 2, 128), f32),
            pltpu.VMEM((4, 8, 8, 2, 128), f32),
            pltpu.VMEM((nblk, foot), f32),
            pltpu.VMEM((nblk, foot), f32),
            pltpu.VMEM((nblk, 64, 128), f32),
            pltpu.VMEM((4, 1024, probe_n), f32),
            pltpu.VMEM((4, 3, 256, probe_n), f32),
            pltpu.VMEM((256, 128), bf16),
            pltpu.VMEM((8, 128), f32),
            pltpu.VMEM((8, 8, 128), f32),
            pltpu.VMEM((8, 128), f32),
            pltpu.VMEM((16, 8, 128), f32),
            pltpu.VMEM((128, 128), f32),
            dma((4,)), dma(()), dma((3, 4)), dma((4, 8)), dma((4, 8)), dma((4, 4)), dma((4,)), dma((4,)),
        ],
        compiler_params=pltpu.CompilerParams(
            collective_id=0, has_side_effects=True, vmem_limit_bytes=60 * 2 ** 20
        ),
        name="exchange",
    )(
        blk_rows.reshape(-1), blk_count.reshape(1, 1), probes.reshape(tile_r * tile_c, probe_n), blk_rows, coef,
        blk_sensor.reshape(1, nblk), owner.reshape(8, 128), weights.reshape(8, 128),
    )
    sens, new, dens = pl.pallas_call(
        finish, out_shape=outs, in_specs=[smem, vmem, vmem], out_specs=(smem, vmem, vmem), name="finish",
    )(sens, new, dens)
    return sens, new.reshape(-1), dens


def solution(mesh):
    in_specs = (
        P("gx", "gy", None),
        P(("gx", "gy"), None),
        P(("gx", "gy")),
        P(("gx", "gy")),
        P(("gx", "gy"), None),
        P(),
        P(),
    )
    out_specs = (P(("gx", "gy")), P(), P("gx", "gy"))
    return jax.shard_map(local, mesh=mesh, in_specs=in_specs, out_specs=out_specs, check_vma=False)
```

```python
import jax
import jax.numpy as jnp
from jax import lax
from jax.experimental import pallas as pl
from jax.experimental.pallas import tpu as pltpu
from jax.sharding import PartitionSpec as P

MESH = pl.DeviceIdType.MESH
HIGHEST = lax.Precision.HIGHEST
FIRST = (0, 1, 2, 2)
SECOND = (1, 2, 0, 0)
THIRD = (2, 0, 1, 1)


def place():
    gx, gy = lax.axis_index("gx"), lax.axis_index("gy")
    return [lax.rem(gx, 4), gx // 4, gy // 2], lax.rem(gy, 2)


def peer(axis, off, core_off):
    at, core = place()
    at[axis] = lax.rem(at[axis] + off, 4)
    return at[1] * 4 + at[0], at[2] * 2 + lax.rem(core + core_off, 2)


def order(i):
    return lax.rem(1 + 2 * i - 3 * (i // 2), 4)


def decode(pos):
    return order(pos // 8), order(lax.rem(pos, 4)), lax.rem(pos, 8) // 4


def kernel(
    rows_h, count_v, probes_h, rows_v, coef_b, ids_r, owner_v, weights_v,
    sens_o, new_o, dens_o,
    rows_s, probes, tile, stage, send, zone, meta, metas, coef_v, ids_v, dens, part, parcel, final, dither, steps_v,
    h_send, h_in, h_mid, h_in2, wide,
    in_sem, row_sem, sent, rs1, rs2, m_sem, fr, h_sem,
):
    n_pts, probe_n = probes.shape
    foot = 128
    chunk = n_pts // 4
    gx, gy = lax.axis_index("gx"), lax.axis_index("gy")
    me = gx * 8 + gy
    at, core = place()
    bf16, f32 = jnp.bfloat16, jnp.float32

    def load(i):
        part_of = pl.ds(i * chunk, chunk)
        return pltpu.make_async_copy(probes_h.at[part_of], probes.at[part_of], in_sem.at[i])

    rows_in = pltpu.make_async_copy(rows_h, rows_s, row_sem)
    for i in range(4):
        load(i).start()
    rows_in.start()
    barrier = pltpu.get_barrier_semaphore()

    def greet(device):
        pl.semaphore_signal(barrier, inc=1, device_id=device, device_id_type=MESH)

    for k in range(1, 16):
        greet((lax.rem(gx // 4 + k // 4, 4) * 4 + lax.rem(lax.rem(gx, 4) + k % 4, 4), gy))
    for k in range(1, 8):
        greet((gx, lax.rem(gy + k, 8)))
    for axis in (0, 1):
        for off in (1, 2, 3):
            greet(peer(axis, off, 1))

    flat = tile.reshape(2 * n_pts, 128)

    def widen(i, c):
        block = probes[pl.ds(pl.multiple_of(i * 64, 64), 64), :].astype(f32)
        flat[pl.ds(i * 128, 64, 2), :] = block[:, :128]
        flat[pl.ds(i * 128 + 1, 64, 2), :] = block[:, 128:]
        return c

    slot_of = lax.broadcasted_iota(jnp.int32, (128, 128), 0)
    coef_v[...] = jnp.where(slot_of < count_v[...], coef_b[...].astype(f32), 0.0)
    names_r = jnp.broadcast_to(ids_r[...].astype(f32), (128, 128))
    meta[:, 0, :] = coef_v[...].T
    meta[:, 1, :] = names_r
    ids_v[...] = names_r.T
    for i in range(4):
        load(i).wait()
        lax.fori_loop(i * (chunk // 64), (i + 1) * (chunk // 64), widen, 0)
    level = (
        lax.rem(lax.broadcasted_iota(jnp.int32, (8, probe_n), 1) * 97, probe_n).astype(f32) + 0.5
    ) * (1.0 / probe_n)
    bell = jnp.where(
        level < 0.5, jnp.sqrt(2.0 * level) - 1.0, 1.0 - jnp.sqrt(jnp.maximum(2.0 - 2.0 * level, 0.0))
    )
    dither[...] = 1.0 + bell * (1.0 / 128)
    rows_in.wait()
    for i in range(16):
        steps_v[i * 16:(i + 1) * 16, :] = (
            lax.broadcasted_iota(jnp.int32, (16, 128), 0) + i * 16
        ).astype(f32).astype(bf16)

    def meta1(k, of, oc):
        first = lax.rem(core + oc, 2) * 64 + k * 16 + lax.rem(at[FIRST[k]] + of, 4) * 4
        src = oc * 4 + of
        return pltpu.make_async_remote_copy(
            src_ref=meta.at[pl.ds(first, 4)], dst_ref=metas.at[k, pl.ds(0, 4), src],
            send_sem=m_sem.at[0, k], recv_sem=m_sem.at[1, k],
            device_id=peer(FIRST[k], of, oc), device_id_type=MESH,
        )

    def meta2(k, og):
        return pltpu.make_async_remote_copy(
            src_ref=metas.at[k, lax.rem(at[SECOND[k]] + og, 4)], dst_ref=metas.at[k, 4 + og],
            send_sem=m_sem.at[2, k], recv_sem=m_sem.at[3, k],
            device_id=peer(SECOND[k], og, 0), device_id_type=MESH,
        )

    def copy1(k, pos):
        og, of, oc = decode(pos)
        return pltpu.make_async_remote_copy(
            src_ref=send.at[k, pos], dst_ref=zone.at[k, og + 3 * ((og + 3) // 4), oc * 4 + of],
            send_sem=sent.at[0, k], recv_sem=rs1.at[k, pos // 4],
            device_id=peer(FIRST[k], of, oc), device_id_type=MESH,
        )

    def copy2(k, og, oc):
        return pltpu.make_async_remote_copy(
            src_ref=zone.at[k, 3 + og, oc * 4:oc * 4 + 4], dst_ref=zone.at[k, og, oc * 4:oc * 4 + 4],
            send_sem=sent.at[1, k], recv_sem=rs2.at[k, og * 2 + oc],
            device_id=peer(SECOND[k], og, 0), device_id_type=MESH,
        )

    def await_bytes(ref, sem):
        pltpu.make_async_copy(ref, ref, sem).wait()

    def copy3(k, oh):
        return pltpu.make_async_remote_copy(
            src_ref=parcel.at[k, oh - 1], dst_ref=final.at[k, oh - 1],
            send_sem=sent.at[2, k], recv_sem=fr.at[k],
            device_id=peer(THIRD[k], oh, 0), device_id_type=MESH,
        )

    others = [(of, oc) for oc in (0, 1) for of in (1, 3, 2, 0) if (of, oc) != (0, 0)]
    for k in range(4):
        metas[k, 0:4, 0] = meta[pl.ds(core * 64 + k * 16 + at[FIRST[k]] * 4, 4)]

    def gather(k, pos, buf):
        og, of, oc = decode(pos)
        chan = (
            lax.rem(core + oc, 2) * 64 + k * 16
            + lax.rem(at[FIRST[k]] + of, 4) * 4 + lax.rem(at[SECOND[k]] + og, 4)
        )
        for i in range(128):
            stage[buf, 2 * i:2 * i + 2, :] = tile[rows_s[chan + i * 128]]
        send[k, pos, :, :128] = stage[buf, pl.ds(0, 128, 2), :].astype(bf16)
        send[k, pos, :, 128:] = stage[buf, pl.ds(1, 128, 2), :].astype(bf16)

    def give(k, pos):
        mine = lax.rem(pos, 8) == 3

        @pl.when(mine)
        def _():
            og, _, _ = decode(pos)
            zone[k, og + 3 * ((og + 3) // 4), 0] = send[k, pos]

        @pl.when(jnp.logical_not(mine))
        def _():
            copy1(k, pos).start()

    def forward(k, i):
        og = order(i)
        for oc in (0, 1):
            await_bytes(zone.at[k, 3 + og, (1 if oc == 0 else 4):oc * 4 + 4], rs1.at[k, 2 * i + oc])
            copy2(k, og, oc).start()

    def first_loop(pos, c):
        for buf, k in enumerate((2, 0)):
            gather(k, pos, buf)
            if buf == 0:
                @pl.when(pos == 1)
                def _():
                    pl.semaphore_wait(barrier, 28)
                    for of, oc in others:
                        for j in range(4):
                            meta1(j, of, oc).start()

                @pl.when(pos == 16)
                def _():
                    for j in range(4):
                        await_bytes(metas.at[j, 0:4, 1:8], m_sem.at[1, j])
                    for og in (1, 3, 2):
                        for j in range(4):
                            meta2(j, og).start()

            @pl.when(pos > 0)
            def _():
                give(k, pos - 1)

        return c

    def second_loop(pos, c):
        for buf, k in enumerate((3, 1)):
            gather(k, pos, buf)
            if buf == 0:
                @pl.when(pos == 0)
                def _():
                    for j in (2, 0):
                        give(j, 31)

                @pl.when(pos == 16)
                def _():
                    forward(2, 1)

            @pl.when(pos > 0)
            def _():
                give(k, pos - 1)

        return c

    lax.fori_loop(0, 32, first_loop, 0)
    forward(2, 0)
    lax.fori_loop(0, 32, second_loop, 0)
    give(3, 31)
    give(1, 31)

    q = lax.broadcasted_iota(jnp.int32, (64, 128), 0)
    hi_of = jnp.where(q < 32, 2 * q, 2 * q - 63)
    lo_of = lax.broadcasted_iota(jnp.int32, (128, 128), 0)

    def spread(first):
        for u in range(4):
            row = rows_v[pl.ds(first + u, 1), :]
            val = coef_v[pl.ds(first + u, 1), :]
            high = jnp.where(row // 128 == hi_of, val, 0.0).astype(bf16)
            low = jnp.where(lax.rem(row, 128) == lo_of, val, 0.0).astype(bf16)
            dens[first + u] = lax.dot_general(
                high, low, (((1,), (1,)), ((), ())), preferred_element_type=f32
            )

    def spread_loop(i, c):
        spread(i * 4)
        return c

    def mix(k, group):
        og, oc = order(group // 2), lax.rem(group, 2)

        @pl.when(group < 6)
        def _():
            await_bytes(zone.at[k, og, pl.ds(oc * 4, 4)], rs2.at[k, og * 2 + oc])

        @pl.when(group == 6)
        def _():
            await_bytes(zone.at[k, 0, 1:4], rs1.at[k, 6])

        @pl.when(group == 7)
        def _():
            await_bytes(zone.at[k, 0, 4:8], rs1.at[k, 7])

        cols = zone[k, og, pl.ds(oc * 4, 4)].reshape(512, probe_n)
        slot = og + 4 * ((og + 3) // 4) + at[SECOND[k]] * (1 - (og + 3) // 4)
        tags = [metas[k, slot, oc * 4 + u] for u in range(4)]
        vals = [jnp.broadcast_to(t[0:1], (16, 128)).astype(bf16) for t in tags]
        zero = jnp.zeros((16, 128), bf16)
        for m in range(4):
            names = [jnp.broadcast_to(t[1:2] - float(m * 256), (16, 128)).astype(bf16) for t in tags]
            mixer = jnp.concatenate(
                [
                    jnp.concatenate(
                        [
                            jnp.where(names[u] == steps_v[i * 16:(i + 1) * 16, :], vals[u], zero)
                            for i in range(16)
                        ],
                        axis=0,
                    )
                    for u in range(4)
                ],
                axis=1,
            )
            part[k, m * 256:(m + 1) * 256, :] += jnp.dot(mixer, cols, preferred_element_type=f32)

    def mix_loop(*kinds):
        def body(i, c):
            for k in kinds:
                mix(k, lax.rem(i + 6, 8))
            return c
        return body

    def sum_up(k):
        for oh in (1, 3, 2):
            block = lax.rem(at[THIRD[k]] + oh, 4)
            rows = part[k, pl.ds(pl.multiple_of(block * 256, 256), 256), :]
            parcel[k, oh - 1] = (rows * dither[0:1, :]).astype(bf16)
        for oh in (1, 3, 2):
            copy3(k, oh).start()

    forward(2, 2)
    for i in range(3):
        forward(0, i)
    forward(1, 0)
    part[...] = jnp.zeros_like(part)
    for k in range(4):
        await_bytes(metas.at[k, 5:8], m_sem.at[3, k])
    lax.fori_loop(0, 16, spread_loop, 0)
    forward(3, 0)
    forward(1, 1)
    lax.fori_loop(16, 32, spread_loop, 0)
    lax.fori_loop(0, 4, mix_loop(2), 0)
    forward(1, 2)
    forward(3, 1)
    lax.fori_loop(4, 8, mix_loop(2), 0)
    sum_up(2)
    lax.fori_loop(0, 4, mix_loop(0), 0)
    forward(3, 2)
    lax.fori_loop(4, 8, mix_loop(0), 0)
    sum_up(0)
    lax.fori_loop(0, 8, mix_loop(1, 3), 0)
    sum_up(1)
    sum_up(3)

    h_send[...] = jnp.zeros_like(h_send)
    ones = jnp.ones((8, 128), f32)
    for k in (2, 0, 1, 3):
        await_bytes(final.at[k], fr.at[k])
        block = at[THIRD[k]]
        whole = part[k, pl.ds(pl.multiple_of(block * 256, 256), 256), :]
        for i in range(3):
            whole = whole + final[k, i].astype(f32)
        whole = whole * whole
        sums = lax.dot_general(
            ones, whole[:, :128] + whole[:, 128:], (((1,), (1,)), ((), ())),
            preferred_element_type=f32, precision=HIGHEST,
        ) * (1.0 / (foot * probe_n))
        for i in range(2):
            h_send[pl.ds(2 * block + i, 1), :] += sums[0:1, i * 128:(i + 1) * 128]

    def first_copy(k):
        to = lax.rem(gy + k, 8)
        return pltpu.make_async_remote_copy(
            src_ref=h_send, dst_ref=h_in.at[gy],
            send_sem=h_sem.at[0], recv_sem=h_sem.at[1],
            device_id=(gx, to), device_id_type=MESH,
        )

    def second_copy(k):
        to = lax.rem(gx // 4 + k // 4, 4) * 4 + lax.rem(lax.rem(gx, 4) + k % 4, 4)
        return pltpu.make_async_remote_copy(
            src_ref=h_mid, dst_ref=h_in2.at[gx],
            send_sem=h_sem.at[2], recv_sem=h_sem.at[3],
            device_id=(to, gy), device_id_type=MESH,
        )

    for k in range(1, 8):
        first_copy(k).start()
    h_in[gy] = h_send[...]
    mine = owner_v[...] == me
    count = jnp.where(mine, 1.0, 0.0)
    before = jnp.where(
        lax.broadcasted_iota(jnp.int32, (128, 128), 0) < lax.broadcasted_iota(jnp.int32, (128, 128), 1),
        1.0, 0.0,
    )
    above = jnp.where(
        lax.broadcasted_iota(jnp.int32, (8, 8), 1) < lax.broadcasted_iota(jnp.int32, (8, 8), 0),
        1.0, 0.0,
    )
    in_row = jnp.dot(count, before, precision=HIGHEST, preferred_element_type=f32)
    rank = in_row + jnp.dot(
        above, jnp.broadcast_to(jnp.sum(count, axis=1, keepdims=True), (8, 128)),
        precision=HIGHEST, preferred_element_type=f32,
    )
    rank = jnp.where(mine, rank, -1.0)
    await_bytes(h_in.at[1:8], h_sem.at[1])
    total = h_in[0]
    for k in range(1, 8):
        total = total + h_in[k]
    h_mid[...] = total
    for k in range(1, 16):
        second_copy(k).start()
    h_in2[gx] = total
    await_bytes(h_in2.at[1:16], h_sem.at[3])
    total = h_in2[0]
    for k in range(1, 16):
        total = total + h_in2[k]

    gain = weights_v[...] * jnp.sqrt(1.0 + total)
    new = 1024.0 * gain / jnp.sum(gain)
    new_o[...] = new
    for k in range(8):
        sens_o[k] = jnp.sum(jnp.where(rank == float(k), total, 0.0))

    ids = ids_v[...]
    lane = lax.broadcasted_iota(jnp.int32, (128, 128), 1)
    picked = jnp.zeros((128, 128), f32)
    for k in range(8):
        picked = picked + jnp.where(ids == (lane + k * 128).astype(f32), new_o[k:k + 1, :], 0.0)
    wide[...] = jnp.broadcast_to(jnp.sum(picked, axis=1, keepdims=True), (128, 128))

    def weigh(i, acc):
        for u in range(8):
            slot = i * 8 + u
            acc = acc + wide[pl.ds(slot, 1), :] * dens[slot]
        return acc

    out = lax.fori_loop(0, 16, weigh, jnp.zeros((64, 128), f32))
    dens_o[:, :128] = out[:32]
    dens_o[:, 128:] = out[32:]

    for k in range(4):
        await_bytes(send.at[k, 0:28], sent.at[0, k])
        await_bytes(zone.at[k, 1:4], sent.at[1, k])
        await_bytes(final.at[k], sent.at[2, k])
        await_bytes(metas.at[k, 0:4, 1:8], m_sem.at[0, k])
        await_bytes(metas.at[k, 5:8], m_sem.at[2, k])
    await_bytes(h_in.at[1:8], h_sem.at[0])
    await_bytes(h_in2.at[1:16], h_sem.at[2])


def finish(sens, new, dens, sens_o, new_o, dens_o):
    for k in range(8):
        sens_o[k] = sens[k]
    new_o[...] = new[...]
    dens_o[...] = dens[...]


def local(probes, blk_rows, blk_sensor, blk_count, coef, owner, weights):
    tile_r, tile_c, probe_n = probes.shape
    nblk, foot = blk_rows.shape
    f32, bf16 = jnp.float32, jnp.bfloat16
    vmem = pl.BlockSpec(memory_space=pltpu.VMEM)
    smem = pl.BlockSpec(memory_space=pltpu.SMEM)
    anyw = pl.BlockSpec(memory_space=pl.ANY)
    dma = pltpu.SemaphoreType.DMA
    outs = (
        jax.ShapeDtypeStruct((8,), f32),
        jax.ShapeDtypeStruct((8, 128), f32),
        jax.ShapeDtypeStruct((tile_r, tile_c), f32),
    )
    sens, new, dens = pl.pallas_call(
        kernel,
        out_shape=outs,
        in_specs=[anyw, vmem, anyw] + [vmem] * 5,
        out_specs=(smem, vmem, vmem),
        scratch_shapes=[
            pltpu.SMEM((nblk * foot,), jnp.int32),
            pltpu.VMEM((tile_r * tile_c, probe_n), bf16),
            pltpu.VMEM((tile_r * tile_c, 2, 128), f32),
            pltpu.VMEM((3, 256, 128), f32),
            pltpu.VMEM((4, 32, nblk, probe_n), bf16),
            pltpu.VMEM((4, 7, 8, nblk, probe_n), bf16),
            pltpu.VMEM((128, 2, 128), f32),
            pltpu.VMEM((4, 8, 8, 2, 128), f32),
            pltpu.VMEM((nblk, foot), f32),
            pltpu.VMEM((nblk, foot), f32),
            pltpu.VMEM((nblk, 64, 128), f32),
            pltpu.VMEM((4, 1024, probe_n), f32),
            pltpu.VMEM((4, 3, 256, probe_n), bf16),
            pltpu.VMEM((4, 3, 256, probe_n), bf16),
            pltpu.VMEM((8, probe_n), f32),
            pltpu.VMEM((256, 128), bf16),
            pltpu.VMEM((8, 128), f32),
            pltpu.VMEM((8, 8, 128), f32),
            pltpu.VMEM((8, 128), f32),
            pltpu.VMEM((16, 8, 128), f32),
            pltpu.VMEM((128, 128), f32),
            dma((4,)), dma(()), dma((3, 4)), dma((4, 8)), dma((4, 8)), dma((4, 4)), dma((4,)), dma((4,)),
        ],
        compiler_params=pltpu.CompilerParams(
            collective_id=0, has_side_effects=True, vmem_limit_bytes=60 * 2 ** 20
        ),
        name="exchange",
    )(
        blk_rows.reshape(-1), blk_count.reshape(1, 1), probes.reshape(tile_r * tile_c, probe_n), blk_rows, coef,
        blk_sensor.reshape(1, nblk), owner.reshape(8, 128), weights.reshape(8, 128),
    )
    sens, new, dens = pl.pallas_call(
        finish, out_shape=outs, in_specs=[smem, vmem, vmem], out_specs=(smem, vmem, vmem), name="finish",
    )(sens, new, dens)
    return sens, new.reshape(-1), dens


def solution(mesh):
    in_specs = (
        P("gx", "gy", None),
        P(("gx", "gy"), None),
        P(("gx", "gy")),
        P(("gx", "gy")),
        P(("gx", "gy"), None),
        P(),
        P(),
    )
    out_specs = (P(("gx", "gy")), P(), P("gx", "gy"))
    return jax.shard_map(local, mesh=mesh, in_specs=in_specs, out_specs=out_specs, check_vma=False)
```

```python
import jax
import jax.numpy as jnp
from jax import lax
from jax.experimental import pallas as pl
from jax.experimental.pallas import tpu as pltpu
from jax.sharding import PartitionSpec as P

MESH = pl.DeviceIdType.MESH
HIGHEST = lax.Precision.HIGHEST
FIRST = (0, 1, 2, 0)
SECOND = (1, 2, 0, 1)
THIRD = (2, 0, 1, 2)
TURN = {2: 0, 1: 1, 3: 2, 0: 3}


def place():
    gx, gy = lax.axis_index("gx"), lax.axis_index("gy")
    return [lax.rem(gx, 4), gx // 4, gy // 2], lax.rem(gy, 2)


def peer(axis, off, core_off):
    at, core = place()
    at[axis] = lax.rem(at[axis] + off, 4)
    return at[1] * 4 + at[0], at[2] * 2 + lax.rem(core + core_off, 2)


def order(i):
    return lax.rem(1 + 2 * i - 3 * (i // 2), 4)


def decode(pos):
    a, b = lax.rem(pos // 8, 2), pos // 16
    return 2 - a + b - 2 * a * b, order(lax.rem(pos, 4)), lax.rem(pos, 8) // 4


def kernel(
    rows_h, count_v, probes_h, rows_v, coef_b, ids_r, owner_v, weights_v,
    sens_o, new_o, dens_o,
    rows_s, probes, tile, stage, send, zone, meta, metas, coef_v, ids_v, dens, part,
    out1, in1, out2, in2, parcel, final, dither, steps_v,
    h_send, h_in, h_mid, h_in2, wide,
    in_sem, row_sem, sent, rs1, r1_sem, r2_sem, m_sem, fr, h_sem,
):
    n_pts, probe_n = probes.shape
    foot = 128
    chunk = n_pts // 4
    gx, gy = lax.axis_index("gx"), lax.axis_index("gy")
    me = gx * 8 + gy
    at, core = place()
    bf16, f32 = jnp.bfloat16, jnp.float32

    def load(i):
        part_of = pl.ds(i * chunk, chunk)
        return pltpu.make_async_copy(probes_h.at[part_of], probes.at[part_of], in_sem.at[i])

    rows_in = pltpu.make_async_copy(rows_h, rows_s, row_sem)
    for i in range(4):
        load(i).start()
    rows_in.start()
    barrier = pltpu.get_barrier_semaphore()

    def greet(device):
        pl.semaphore_signal(barrier, inc=1, device_id=device, device_id_type=MESH)

    for k in range(1, 16):
        greet((lax.rem(gx // 4 + k // 4, 4) * 4 + lax.rem(lax.rem(gx, 4) + k % 4, 4), gy))
    for k in range(1, 8):
        greet((gx, lax.rem(gy + k, 8)))
    for axis in (0, 1):
        for off in (1, 2, 3):
            greet(peer(axis, off, 1))

    flat = tile.reshape(2 * n_pts, 128)

    def widen(i, c):
        block = probes[pl.ds(pl.multiple_of(i * 64, 64), 64), :].astype(f32)
        flat[pl.ds(i * 128, 64, 2), :] = block[:, :128]
        flat[pl.ds(i * 128 + 1, 64, 2), :] = block[:, 128:]
        return c

    slot_of = lax.broadcasted_iota(jnp.int32, (128, 128), 0)
    coef_v[...] = jnp.where(slot_of < count_v[...], coef_b[...].astype(f32), 0.0)
    names_r = jnp.broadcast_to(ids_r[...].astype(f32), (128, 128))
    meta[:, 0, :] = coef_v[...].T
    meta[:, 1, :] = names_r
    ids_v[...] = names_r.T
    for i in range(4):
        load(i).wait()
        lax.fori_loop(i * (chunk // 64), (i + 1) * (chunk // 64), widen, 0)
    level = (
        lax.rem(lax.broadcasted_iota(jnp.int32, (8, probe_n), 1) * 97, probe_n).astype(f32) + 0.5
    ) * (1.0 / probe_n)
    bell = jnp.where(
        level < 0.5, jnp.sqrt(2.0 * level) - 1.0, 1.0 - jnp.sqrt(jnp.maximum(2.0 - 2.0 * level, 0.0))
    )
    dither[...] = 1.0 + bell * (1.0 / 128)
    rows_in.wait()
    for i in range(16):
        steps_v[i * 16:(i + 1) * 16, :] = (
            lax.broadcasted_iota(jnp.int32, (16, 128), 0) + i * 16
        ).astype(f32).astype(bf16)

    def meta1(k, of, oc):
        first = lax.rem(core + oc, 2) * 64 + k * 16 + lax.rem(at[FIRST[k]] + of, 4) * 4
        src = oc * 4 + of
        return pltpu.make_async_remote_copy(
            src_ref=meta.at[pl.ds(first, 4)], dst_ref=metas.at[k, pl.ds(0, 4), src],
            send_sem=m_sem.at[0, k], recv_sem=m_sem.at[1, k],
            device_id=peer(FIRST[k], of, oc), device_id_type=MESH,
        )

    def copy1(k, pos):
        og, of, oc = decode(pos)
        return pltpu.make_async_remote_copy(
            src_ref=send.at[k, pos], dst_ref=zone.at[k, og, oc * 4 + of],
            send_sem=sent.at[0, k], recv_sem=rs1.at[k, pos // 4],
            device_id=peer(FIRST[k], of, oc), device_id_type=MESH,
        )

    def ring1(k, half):
        return pltpu.make_async_remote_copy(
            src_ref=out1.at[k, half], dst_ref=in1.at[k, half],
            send_sem=sent.at[1, k], recv_sem=r1_sem.at[k, half],
            device_id=peer(SECOND[k], 1 + 2 * half, 0), device_id_type=MESH,
        )

    def ring2(k, half):
        return pltpu.make_async_remote_copy(
            src_ref=out2.at[k, half], dst_ref=in2.at[k, half],
            send_sem=sent.at[3, k], recv_sem=r2_sem.at[k, half],
            device_id=peer(SECOND[k], 1 + 2 * half, 0), device_id_type=MESH,
        )

    def await_bytes(ref, sem):
        pltpu.make_async_copy(ref, ref, sem).wait()

    def copy3(k, oh):
        return pltpu.make_async_remote_copy(
            src_ref=parcel.at[k, oh - 1], dst_ref=final.at[k, oh - 1],
            send_sem=sent.at[2, k], recv_sem=fr.at[k],
            device_id=peer(THIRD[k], oh, 0), device_id_type=MESH,
        )

    others = [(of, oc) for oc in (0, 1) for of in (1, 3, 2, 0) if (of, oc) != (0, 0)]
    for k in range(4):
        metas[k, 0:4, 0] = meta[pl.ds(core * 64 + k * 16 + at[FIRST[k]] * 4, 4)]

    def gather(k, pos, buf):
        og, of, oc = decode(pos)
        chan = (
            lax.rem(core + oc, 2) * 64 + k * 16
            + lax.rem(at[FIRST[k]] + of, 4) * 4 + lax.rem(at[SECOND[k]] + og, 4)
        )
        for i in range(128):
            stage[buf, 2 * i:2 * i + 2, :] = tile[rows_s[chan + i * 128]]
        send[k, pos, :, :128] = stage[buf, pl.ds(0, 128, 2), :].astype(bf16)
        send[k, pos, :, 128:] = stage[buf, pl.ds(1, 128, 2), :].astype(bf16)

    def give(k, pos):
        mine = lax.rem(pos, 8) == 3

        @pl.when(mine)
        def _():
            og, _, _ = decode(pos)
            zone[k, og, 0] = send[k, pos]

        @pl.when(jnp.logical_not(mine))
        def _():
            copy1(k, pos).start()

    def first_loop(pos, c):
        for buf, k in enumerate((2, 0, 1)):
            gather(k, pos, buf)
            if buf == 0:
                @pl.when(pos == 1)
                def _():
                    pl.semaphore_wait(barrier, 28)
                    for of, oc in others:
                        for j in range(4):
                            meta1(j, of, oc).start()

            @pl.when(pos > 0)
            def _():
                give(k, pos - 1)

        return c

    def second_loop(pos, c):
        gather(3, pos, 0)

        @pl.when(pos > 0)
        def _():
            give(3, pos - 1)

        return c

    q = lax.broadcasted_iota(jnp.int32, (64, 128), 0)
    hi_of = jnp.where(q < 32, 2 * q, 2 * q - 63)
    lo_of = lax.broadcasted_iota(jnp.int32, (128, 128), 0)

    def spread(first):
        for u in range(4):
            row = rows_v[pl.ds(first + u, 1), :]
            val = coef_v[pl.ds(first + u, 1), :]
            high = jnp.where(row // 128 == hi_of, val, 0.0).astype(bf16)
            low = jnp.where(lax.rem(row, 128) == lo_of, val, 0.0).astype(bf16)
            dens[first + u] = lax.dot_general(
                high, low, (((1,), (1,)), ((), ())), preferred_element_type=f32
            )

    def spread_loop(i, c):
        spread(i * 4)
        return c

    def mix(k, og, into):
        turn = TURN[og]
        await_bytes(zone.at[k, og, 1:4], rs1.at[k, 2 * turn])
        await_bytes(zone.at[k, og, 4:8], rs1.at[k, 2 * turn + 1])
        chan = lax.rem(at[SECOND[k]] + og, 4)
        zero = jnp.zeros((16, 128), bf16)

        def block(m):
            total = None
            for oc in range(2):
                tags = [metas[k, chan, oc * 4 + u] for u in range(4)]
                vals = [jnp.broadcast_to(t[0:1], (16, 128)).astype(bf16) for t in tags]
                base = (jnp.int32(m) * 256).astype(f32)
                names = [jnp.broadcast_to(t[1:2] - base, (16, 128)).astype(bf16) for t in tags]
                mixer = jnp.concatenate(
                    [
                        jnp.concatenate(
                            [
                                jnp.where(names[u] == steps_v[i * 16:(i + 1) * 16, :], vals[u], zero)
                                for i in range(16)
                            ],
                            axis=0,
                        )
                        for u in range(4)
                    ],
                    axis=1,
                )
                cols = zone[k, og, oc * 4:oc * 4 + 4].reshape(512, probe_n)
                got = jnp.dot(mixer, cols, preferred_element_type=f32)
                total = got if total is None else total + got
            into(m, total)

        def body(i, c):
            for u in range(4):
                block(i * 4 + u)
            return c

        lax.fori_loop(0, 4 // 4, body, 0)

    def rows_at(m):
        return pl.ds(pl.multiple_of(m * 256, 256), 256)

    def step1(k):
        def into(m, total):
            total = total * dither[0:1, :]
            out1[k, 0, rows_at(m), :] = total[:, :128].astype(bf16)
            out1[k, 1, rows_at(m), :] = total[:, 128:].astype(bf16)

        mix(k, 2, into)
        ring1(k, 0).start()
        ring1(k, 1).start()

    def step2(k):
        for half in (0, 1):
            def into(m, total):
                other = in1[k, half, rows_at(m), :].astype(f32)
                left, right = total[:, :128], total[:, 128:]
                if half == 0:
                    left = left + other
                else:
                    right = right + other
                out2[k, half, rows_at(m), :128] = (left * dither[0:1, :128]).astype(bf16)
                out2[k, half, rows_at(m), 128:] = (right * dither[0:1, 128:]).astype(bf16)

            await_bytes(in1.at[k, half], r1_sem.at[k, half])
            mix(k, 1 + 2 * half, into)
            ring2(k, half).start()

    def own(k):
        def into(m, total):
            part[k, rows_at(m), :] = total

        mix(k, 0, into)

    def collect(k):
        for half in (0, 1):
            await_bytes(in2.at[k, half], r2_sem.at[k, half])

    def sum_up(k):
        for oh in (1, 3, 2):
            block = rows_at(lax.rem(at[THIRD[k]] + oh, 4))
            rows = part[k, block, :] + in2[k, 0, block, :].astype(f32) + in2[k, 1, block, :].astype(f32)
            parcel[k, oh - 1] = (rows * dither[0:1, :]).astype(bf16)
        for oh in (1, 3, 2):
            copy3(k, oh).start()

    lax.fori_loop(0, 32, first_loop, 0)
    for k in (2, 0, 1):
        give(k, 31)
    for k in range(4):
        await_bytes(metas.at[k, 0:4, 1:8], m_sem.at[1, k])
    step1(2)
    step1(1)
    step1(0)
    lax.fori_loop(0, 32, second_loop, 0)
    give(3, 31)
    step2(1)
    step2(0)
    step2(2)
    step1(3)
    own(1)
    own(0)
    lax.fori_loop(0, 16, spread_loop, 0)
    collect(1)
    sum_up(1)
    collect(0)
    sum_up(0)
    step2(3)
    own(2)
    own(3)
    lax.fori_loop(16, 32, spread_loop, 0)
    collect(2)
    sum_up(2)
    collect(3)
    sum_up(3)

    h_send[...] = jnp.zeros_like(h_send)
    ones = jnp.ones((8, 128), f32)
    for k in (0, 1, 2, 3):
        await_bytes(final.at[k], fr.at[k])
        block = at[THIRD[k]]
        whole = part[k, rows_at(block), :]
        for half in (0, 1):
            whole = whole + in2[k, half, rows_at(block), :].astype(f32)
        for i in range(3):
            whole = whole + final[k, i].astype(f32)
        whole = whole * whole
        sums = lax.dot_general(
            ones, whole[:, :128] + whole[:, 128:], (((1,), (1,)), ((), ())),
            preferred_element_type=f32, precision=HIGHEST,
        ) * (1.0 / (foot * probe_n))
        for i in range(2):
            h_send[pl.ds(2 * block + i, 1), :] += sums[0:1, i * 128:(i + 1) * 128]

    def first_copy(k):
        to = lax.rem(gy + k, 8)
        return pltpu.make_async_remote_copy(
            src_ref=h_send, dst_ref=h_in.at[gy],
            send_sem=h_sem.at[0], recv_sem=h_sem.at[1],
            device_id=(gx, to), device_id_type=MESH,
        )

    def second_copy(k):
        to = lax.rem(gx // 4 + k // 4, 4) * 4 + lax.rem(lax.rem(gx, 4) + k % 4, 4)
        return pltpu.make_async_remote_copy(
            src_ref=h_mid, dst_ref=h_in2.at[gx],
            send_sem=h_sem.at[2], recv_sem=h_sem.at[3],
            device_id=(to, gy), device_id_type=MESH,
        )

    for k in range(1, 8):
        first_copy(k).start()
    h_in[gy] = h_send[...]
    mine = owner_v[...] == me
    count = jnp.where(mine, 1.0, 0.0)
    before = jnp.where(
        lax.broadcasted_iota(jnp.int32, (128, 128), 0) < lax.broadcasted_iota(jnp.int32, (128, 128), 1),
        1.0, 0.0,
    )
    above = jnp.where(
        lax.broadcasted_iota(jnp.int32, (8, 8), 1) < lax.broadcasted_iota(jnp.int32, (8, 8), 0),
        1.0, 0.0,
    )
    in_row = jnp.dot(count, before, precision=HIGHEST, preferred_element_type=f32)
    rank = in_row + jnp.dot(
        above, jnp.broadcast_to(jnp.sum(count, axis=1, keepdims=True), (8, 128)),
        precision=HIGHEST, preferred_element_type=f32,
    )
    rank = jnp.where(mine, rank, -1.0)
    await_bytes(h_in.at[1:8], h_sem.at[1])
    total = h_in[0]
    for k in range(1, 8):
        total = total + h_in[k]
    h_mid[...] = total
    for k in range(1, 16):
        second_copy(k).start()
    h_in2[gx] = total
    await_bytes(h_in2.at[1:16], h_sem.at[3])
    total = h_in2[0]
    for k in range(1, 16):
        total = total + h_in2[k]

    gain = weights_v[...] * jnp.sqrt(1.0 + total)
    new = 1024.0 * gain / jnp.sum(gain)
    new_o[...] = new
    for k in range(8):
        sens_o[k] = jnp.sum(jnp.where(rank == float(k), total, 0.0))

    ids = ids_v[...]
    lane = lax.broadcasted_iota(jnp.int32, (128, 128), 1)
    picked = jnp.zeros((128, 128), f32)
    for k in range(8):
        picked = picked + jnp.where(ids == (lane + k * 128).astype(f32), new_o[k:k + 1, :], 0.0)
    wide[...] = jnp.broadcast_to(jnp.sum(picked, axis=1, keepdims=True), (128, 128))

    def weigh(i, acc):
        for u in range(8):
            slot = i * 8 + u
            acc = acc + wide[pl.ds(slot, 1), :] * dens[slot]
        return acc

    out = lax.fori_loop(0, 16, weigh, jnp.zeros((64, 128), f32))
    dens_o[:, :128] = out[:32]
    dens_o[:, 128:] = out[32:]

    for k in range(4):
        await_bytes(send.at[k, 0:28], sent.at[0, k])
        await_bytes(in1.at[k], sent.at[1, k])
        await_bytes(in2.at[k], sent.at[3, k])
        await_bytes(final.at[k], sent.at[2, k])
        await_bytes(metas.at[k, 0:4, 1:8], m_sem.at[0, k])
    await_bytes(h_in.at[1:8], h_sem.at[0])
    await_bytes(h_in2.at[1:16], h_sem.at[2])


def finish(sens, new, dens, sens_o, new_o, dens_o):
    for k in range(8):
        sens_o[k] = sens[k]
    new_o[...] = new[...]
    dens_o[...] = dens[...]


def local(probes, blk_rows, blk_sensor, blk_count, coef, owner, weights):
    tile_r, tile_c, probe_n = probes.shape
    nblk, foot = blk_rows.shape
    f32, bf16 = jnp.float32, jnp.bfloat16
    vmem = pl.BlockSpec(memory_space=pltpu.VMEM)
    smem = pl.BlockSpec(memory_space=pltpu.SMEM)
    anyw = pl.BlockSpec(memory_space=pl.ANY)
    dma = pltpu.SemaphoreType.DMA
    outs = (
        jax.ShapeDtypeStruct((8,), f32),
        jax.ShapeDtypeStruct((8, 128), f32),
        jax.ShapeDtypeStruct((tile_r, tile_c), f32),
    )
    sens, new, dens = pl.pallas_call(
        kernel,
        out_shape=outs,
        in_specs=[anyw, vmem, anyw] + [vmem] * 5,
        out_specs=(smem, vmem, vmem),
        scratch_shapes=[
            pltpu.SMEM((nblk * foot,), jnp.int32),
            pltpu.VMEM((tile_r * tile_c, probe_n), bf16),
            pltpu.VMEM((tile_r * tile_c, 2, 128), f32),
            pltpu.VMEM((3, 256, 128), f32),
            pltpu.VMEM((4, 32, nblk, probe_n), bf16),
            pltpu.VMEM((4, 4, 8, nblk, probe_n), bf16),
            pltpu.VMEM((128, 2, 128), f32),
            pltpu.VMEM((4, 4, 8, 2, 128), f32),
            pltpu.VMEM((nblk, foot), f32),
            pltpu.VMEM((nblk, foot), f32),
            pltpu.VMEM((nblk, 64, 128), f32),
            pltpu.VMEM((4, 1024, probe_n), f32),
            pltpu.VMEM((4, 2, 1024, 128), bf16),
            pltpu.VMEM((4, 2, 1024, 128), bf16),
            pltpu.VMEM((4, 2, 1024, probe_n), bf16),
            pltpu.VMEM((4, 2, 1024, probe_n), bf16),
            pltpu.VMEM((4, 3, 256, probe_n), bf16),
            pltpu.VMEM((4, 3, 256, probe_n), bf16),
            pltpu.VMEM((8, probe_n), f32),
            pltpu.VMEM((256, 128), bf16),
            pltpu.VMEM((8, 128), f32),
            pltpu.VMEM((8, 8, 128), f32),
            pltpu.VMEM((8, 128), f32),
            pltpu.VMEM((16, 8, 128), f32),
            pltpu.VMEM((128, 128), f32),
            dma((4,)), dma(()), dma((4, 4)), dma((4, 8)), dma((4, 2)), dma((4, 2)), dma((2, 4)), dma((4,)), dma((4,)),
        ],
        compiler_params=pltpu.CompilerParams(
            collective_id=0, has_side_effects=True, vmem_limit_bytes=60 * 2 ** 20
        ),
        name="exchange",
    )(
        blk_rows.reshape(-1), blk_count.reshape(1, 1), probes.reshape(tile_r * tile_c, probe_n), blk_rows, coef,
        blk_sensor.reshape(1, nblk), owner.reshape(8, 128), weights.reshape(8, 128),
    )
    sens, new, dens = pl.pallas_call(
        finish, out_shape=outs, in_specs=[smem, vmem, vmem], out_specs=(smem, vmem, vmem), name="finish",
    )(sens, new, dens)
    return sens, new.reshape(-1), dens


def solution(mesh):
    in_specs = (
        P("gx", "gy", None),
        P(("gx", "gy"), None),
        P(("gx", "gy")),
        P(("gx", "gy")),
        P(("gx", "gy"), None),
        P(),
        P(),
    )
    out_specs = (P(("gx", "gy")), P(), P("gx", "gy"))
    return jax.shard_map(local, mesh=mesh, in_specs=in_specs, out_specs=out_specs, check_vma=False)
```

```python
import jax
import jax.numpy as jnp
from jax import lax
from jax.experimental import pallas as pl
from jax.experimental.pallas import tpu as pltpu
from jax.sharding import PartitionSpec as P

MESH = pl.DeviceIdType.MESH
HIGHEST = lax.Precision.HIGHEST
FIRST = (0, 1, 2, 0, 2)
SECOND = (1, 2, 0, 1, 1)
THIRD = (2, 0, 1, 2, 0)
BASE = (0, 16, 32, 48, 48)
KINDS = (0, 1, 2, 3, 4)
TURN = {2: 0, 1: 1, 3: 2, 0: 3}


def place():
    gx, gy = lax.axis_index("gx"), lax.axis_index("gy")
    return [lax.rem(gx, 4), gx // 4, gy // 2], lax.rem(gy, 2)


def peer(axis, off, core_off):
    at, core = place()
    at[axis] = lax.rem(at[axis] + off, 4)
    return at[1] * 4 + at[0], at[2] * 2 + lax.rem(core + core_off, 2)


def order(i):
    return lax.rem(1 + 2 * i - 3 * (i // 2), 4)


def decode(pos):
    a, b = lax.rem(pos // 8, 2), pos // 16
    return 2 - a + b - 2 * a * b, order(lax.rem(pos, 4)), lax.rem(pos, 8) // 4


def kernel(
    rows_h, count_v, probes_h, rows_v, coef_b, ids_r, owner_v, weights_v,
    sens_o, new_o, dens_o,
    rows_s, probes, tile, stage, meta, metas, coef_v, ids_v, dens, dither, steps_v,
    send_w, zone_w, part_w, out1_w, in1_w, out2_w, in2_w, parcel_w, final_w,
    send_n, zone_n, part_n, out1_n, in1_n, out2_n, in2_n, parcel_n, final_n,
    h_send, h_in, h_mid, h_in2, wide,
    in_sem, row_sem, sent, rs1, r1_sem, r2_sem, m_sem, fr, h_sem,
):
    n_pts, probe_n = probes.shape
    foot = 128
    chunk = n_pts // 4
    gx, gy = lax.axis_index("gx"), lax.axis_index("gy")
    me = gx * 8 + gy
    at, core = place()
    bf16, f32 = jnp.bfloat16, jnp.float32

    def by_kind(wide_ref, narrow_ref):
        return [wide_ref.at[i] for i in range(3)] + [narrow_ref.at[i] for i in range(2)]

    send, zone, part = by_kind(send_w, send_n), by_kind(zone_w, zone_n), by_kind(part_w, part_n)
    out1, in1 = by_kind(out1_w, out1_n), by_kind(in1_w, in1_n)
    out2, in2 = by_kind(out2_w, out2_n), by_kind(in2_w, in2_n)
    parcel, final = by_kind(parcel_w, parcel_n), by_kind(final_w, final_n)
    lanes = [slice(0, 256)] * 3 + [slice(0, 128), slice(128, 256)]

    def load(i):
        part_of = pl.ds(i * chunk, chunk)
        return pltpu.make_async_copy(probes_h.at[part_of], probes.at[part_of], in_sem.at[i])

    rows_in = pltpu.make_async_copy(rows_h, rows_s, row_sem)
    for i in range(4):
        load(i).start()
    rows_in.start()
    barrier = pltpu.get_barrier_semaphore()

    def greet(device):
        pl.semaphore_signal(barrier, inc=1, device_id=device, device_id_type=MESH)

    for k in range(1, 16):
        greet((lax.rem(gx // 4 + k // 4, 4) * 4 + lax.rem(lax.rem(gx, 4) + k % 4, 4), gy))
    for k in range(1, 8):
        greet((gx, lax.rem(gy + k, 8)))
    for axis in (0, 1):
        for off in (1, 2, 3):
            greet(peer(axis, off, 1))

    flat = tile.reshape(2 * n_pts, 128)

    def widen(i, c):
        block = probes[pl.ds(pl.multiple_of(i * 64, 64), 64), :].astype(f32)
        flat[pl.ds(i * 128, 64, 2), :] = block[:, :128]
        flat[pl.ds(i * 128 + 1, 64, 2), :] = block[:, 128:]
        return c

    slot_of = lax.broadcasted_iota(jnp.int32, (128, 128), 0)
    coef_v[...] = jnp.where(slot_of < count_v[...], coef_b[...].astype(f32), 0.0)
    names_r = jnp.broadcast_to(ids_r[...].astype(f32), (128, 128))
    meta[:, 0, :] = coef_v[...].T
    meta[:, 1, :] = names_r
    ids_v[...] = names_r.T
    for i in range(4):
        load(i).wait()
        lax.fori_loop(i * (chunk // 64), (i + 1) * (chunk // 64), widen, 0)
    level = (
        lax.rem(lax.broadcasted_iota(jnp.int32, (8, probe_n), 1) * 97, probe_n).astype(f32) + 0.5
    ) * (1.0 / probe_n)
    bell = jnp.where(
        level < 0.5, jnp.sqrt(2.0 * level) - 1.0, 1.0 - jnp.sqrt(jnp.maximum(2.0 - 2.0 * level, 0.0))
    )
    dither[...] = 1.0 + bell * (1.0 / 128)
    rows_in.wait()
    for i in range(16):
        steps_v[i * 16:(i + 1) * 16, :] = (
            lax.broadcasted_iota(jnp.int32, (16, 128), 0) + i * 16
        ).astype(f32).astype(bf16)

    def meta1(k, of, oc):
        first = lax.rem(core + oc, 2) * 64 + BASE[k] + lax.rem(at[FIRST[k]] + of, 4) * 4
        src = oc * 4 + of
        return pltpu.make_async_remote_copy(
            src_ref=meta.at[pl.ds(first, 4)], dst_ref=metas.at[k, pl.ds(0, 4), src],
            send_sem=m_sem.at[0, k], recv_sem=m_sem.at[1, k],
            device_id=peer(FIRST[k], of, oc), device_id_type=MESH,
        )

    def copy1(k, pos):
        og, of, oc = decode(pos)
        return pltpu.make_async_remote_copy(
            src_ref=send[k].at[pos], dst_ref=zone[k].at[og, oc * 4 + of],
            send_sem=sent.at[0, k], recv_sem=rs1.at[k, pos // 4],
            device_id=peer(FIRST[k], of, oc), device_id_type=MESH,
        )

    def ring1(k, half):
        return pltpu.make_async_remote_copy(
            src_ref=out1[k].at[half], dst_ref=in1[k].at[half],
            send_sem=sent.at[1, k], recv_sem=r1_sem.at[k, half],
            device_id=peer(SECOND[k], 1 + 2 * half, 0), device_id_type=MESH,
        )

    def ring2(k, half):
        return pltpu.make_async_remote_copy(
            src_ref=out2[k].at[half], dst_ref=in2[k].at[half],
            send_sem=sent.at[3, k], recv_sem=r2_sem.at[k, half],
            device_id=peer(SECOND[k], 1 + 2 * half, 0), device_id_type=MESH,
        )

    def await_bytes(ref, sem):
        pltpu.make_async_copy(ref, ref, sem).wait()

    def copy3(k, oh):
        return pltpu.make_async_remote_copy(
            src_ref=parcel[k].at[oh - 1], dst_ref=final[k].at[oh - 1],
            send_sem=sent.at[2, k], recv_sem=fr.at[k],
            device_id=peer(THIRD[k], oh, 0), device_id_type=MESH,
        )

    others = [(of, oc) for oc in (0, 1) for of in (1, 3, 2, 0) if (of, oc) != (0, 0)]
    for k in KINDS:
        metas[k, 0:4, 0] = meta[pl.ds(core * 64 + BASE[k] + at[FIRST[k]] * 4, 4)]

    def gather(k, pos, buf):
        og, of, oc = decode(pos)
        chan = (
            lax.rem(core + oc, 2) * 64 + BASE[k]
            + lax.rem(at[FIRST[k]] + of, 4) * 4 + lax.rem(at[SECOND[k]] + og, 4)
        )
        for i in range(128):
            stage[buf, 2 * i:2 * i + 2, :] = tile[rows_s[chan + i * 128]]
        left = stage[buf, pl.ds(0, 128, 2), :].astype(bf16)
        right = stage[buf, pl.ds(1, 128, 2), :].astype(bf16)
        if k < 3:
            send[k][pos, :, :128] = left
            send[k][pos, :, 128:] = right
        else:
            send[3][pos] = left
            send[4][twin(pos)] = right

    def twin(pos):
        _, of, _ = decode(pos)
        of = lax.rem(of + at[0] - at[2] + 4, 4)
        a, b = lax.rem(of, 2), of // 2
        return pos // 4 * 4 + 3 - 3 * a - b + 2 * a * b

    def give(k, pos):
        mine = lax.rem(pos, 8) == 3

        @pl.when(mine)
        def _():
            og, _, _ = decode(pos)
            zone[k][og, 0] = send[k][pos]

        @pl.when(jnp.logical_not(mine))
        def _():
            copy1(k, pos).start()

    def first_loop(pos, c):
        for buf, k in enumerate((2, 0, 1)):
            gather(k, pos, buf)
            if buf == 0:
                @pl.when(pos == 1)
                def _():
                    pl.semaphore_wait(barrier, 28)
                    for of, oc in others:
                        for j in KINDS:
                            meta1(j, of, oc).start()

            @pl.when(pos > 0)
            def _():
                give(k, pos - 1)

        return c

    def second_loop(pos, c):
        gather(3, pos, 0)

        @pl.when(pos > 0)
        def _():
            give(3, pos - 1)
            give(4, twin(pos - 1))

        return c

    q = lax.broadcasted_iota(jnp.int32, (64, 128), 0)
    hi_of = jnp.where(q < 32, 2 * q, 2 * q - 63)
    lo_of = lax.broadcasted_iota(jnp.int32, (128, 128), 0)

    def spread(first):
        for u in range(4):
            row = rows_v[pl.ds(first + u, 1), :]
            val = coef_v[pl.ds(first + u, 1), :]
            high = jnp.where(row // 128 == hi_of, val, 0.0).astype(bf16)
            low = jnp.where(lax.rem(row, 128) == lo_of, val, 0.0).astype(bf16)
            dens[first + u] = lax.dot_general(
                high, low, (((1,), (1,)), ((), ())), preferred_element_type=f32
            )

    def spread_loop(i, c):
        spread(i * 4)
        return c

    def mix(k, og, into):
        turn = TURN[og]
        await_bytes(zone[k].at[og, 1:4], rs1.at[k, 2 * turn])
        await_bytes(zone[k].at[og, 4:8], rs1.at[k, 2 * turn + 1])
        chan = lax.rem(at[SECOND[k]] + og, 4)
        zero = jnp.zeros((16, 128), bf16)

        for m in range(4):
            total = None
            for oc in range(2):
                tags = [metas[k, chan, oc * 4 + u] for u in range(4)]
                vals = [jnp.broadcast_to(t[0:1], (16, 128)).astype(bf16) for t in tags]
                base = float(m * 256)
                names = [jnp.broadcast_to(t[1:2] - base, (16, 128)).astype(bf16) for t in tags]
                mixer = jnp.concatenate(
                    [
                        jnp.concatenate(
                            [
                                jnp.where(names[u] == steps_v[i * 16:(i + 1) * 16, :], vals[u], zero)
                                for i in range(16)
                            ],
                            axis=0,
                        )
                        for u in range(4)
                    ],
                    axis=1,
                )
                cols = zone[k][og, oc * 4:oc * 4 + 4].reshape(512, 256 if k < 3 else 128)
                got = jnp.dot(mixer, cols, preferred_element_type=f32)
                total = got if total is None else total + got
            into(m, total)

    def rows_at(m):
        return pl.ds(pl.multiple_of(m * 256, 256), 256)

    def step1(k):
        def into(m, total):
            out1[k][m // 2, m % 2 * 256:m % 2 * 256 + 256, :] = (
                total * dither[0:1, lanes[k]]
            ).astype(bf16)

        mix(k, 2, into)
        ring1(k, 0).start()
        ring1(k, 1).start()

    def step2(k):
        for half in (0, 1):
            def into(m, total):
                if m // 2 == half:
                    total = total + in1[k][half, m % 2 * 256:m % 2 * 256 + 256, :].astype(f32)
                out2[k][half, m * 256:m * 256 + 256, :] = (total * dither[0:1, lanes[k]]).astype(bf16)

            await_bytes(in1[k].at[half], r1_sem.at[k, half])
            mix(k, 1 + 2 * half, into)
            ring2(k, half).start()

    def own(k):
        def into(m, total):
            part[k][m * 256:m * 256 + 256, :] = total

        mix(k, 0, into)

    def collect(k):
        for half in (0, 1):
            await_bytes(in2[k].at[half], r2_sem.at[k, half])

    def summed(k, block):
        rows = part[k][rows_at(block), :]
        for half in (0, 1):
            rows = rows + in2[k][half, rows_at(block), :].astype(f32)
        return rows

    def sum_up(k):
        for oh in (1, 3, 2):
            rows = summed(k, lax.rem(at[THIRD[k]] + oh, 4))
            parcel[k][oh - 1] = (rows * dither[0:1, lanes[k]]).astype(bf16)
        for oh in (1, 3, 2):
            copy3(k, oh).start()

    lax.fori_loop(0, 32, first_loop, 0)
    for k in (2, 0, 1):
        give(k, 31)
    for k in KINDS:
        await_bytes(metas.at[k, 0:4, 1:8], m_sem.at[1, k])
    step1(2)
    step1(1)
    step1(0)
    lax.fori_loop(0, 32, second_loop, 0)
    give(3, 31)
    give(4, twin(31))
    step2(0)
    step2(1)
    step2(2)
    step1(3)
    step1(4)
    own(1)
    own(0)
    lax.fori_loop(0, 16, spread_loop, 0)
    own(2)
    lax.fori_loop(16, 32, spread_loop, 0)
    collect(0)
    sum_up(0)
    step2(3)
    step2(4)
    own(3)
    own(4)
    collect(1)
    sum_up(1)
    collect(2)
    sum_up(2)
    collect(3)
    sum_up(3)
    collect(4)
    sum_up(4)

    h_send[...] = jnp.zeros_like(h_send)
    ones = jnp.ones((8, 128), f32)
    for k in KINDS:
        await_bytes(final[k], fr.at[k])
        block = at[THIRD[k]]
        whole = summed(k, block)
        for i in range(3):
            whole = whole + final[k][i].astype(f32)
        whole = whole * whole
        if k < 3:
            whole = whole[:, :128] + whole[:, 128:]
        sums = lax.dot_general(
            ones, whole, (((1,), (1,)), ((), ())),
            preferred_element_type=f32, precision=HIGHEST,
        ) * (1.0 / (foot * probe_n))
        for i in range(2):
            h_send[pl.ds(2 * block + i, 1), :] += sums[0:1, i * 128:(i + 1) * 128]

    def first_copy(k):
        to = lax.rem(gy + k, 8)
        return pltpu.make_async_remote_copy(
            src_ref=h_send, dst_ref=h_in.at[gy],
            send_sem=h_sem.at[0], recv_sem=h_sem.at[1],
            device_id=(gx, to), device_id_type=MESH,
        )

    def second_copy(k):
        to = lax.rem(gx // 4 + k // 4, 4) * 4 + lax.rem(lax.rem(gx, 4) + k % 4, 4)
        return pltpu.make_async_remote_copy(
            src_ref=h_mid, dst_ref=h_in2.at[gx],
            send_sem=h_sem.at[2], recv_sem=h_sem.at[3],
            device_id=(to, gy), device_id_type=MESH,
        )

    for k in range(1, 8):
        first_copy(k).start()
    h_in[gy] = h_send[...]
    mine = owner_v[...] == me
    count = jnp.where(mine, 1.0, 0.0)
    before = jnp.where(
        lax.broadcasted_iota(jnp.int32, (128, 128), 0) < lax.broadcasted_iota(jnp.int32, (128, 128), 1),
        1.0, 0.0,
    )
    above = jnp.where(
        lax.broadcasted_iota(jnp.int32, (8, 8), 1) < lax.broadcasted_iota(jnp.int32, (8, 8), 0),
        1.0, 0.0,
    )
    in_row = jnp.dot(count, before, precision=HIGHEST, preferred_element_type=f32)
    rank = in_row + jnp.dot(
        above, jnp.broadcast_to(jnp.sum(count, axis=1, keepdims=True), (8, 128)),
        precision=HIGHEST, preferred_element_type=f32,
    )
    rank = jnp.where(mine, rank, -1.0)
    await_bytes(h_in.at[1:8], h_sem.at[1])
    total = h_in[0]
    for k in range(1, 8):
        total = total + h_in[k]
    h_mid[...] = total
    for k in range(1, 16):
        second_copy(k).start()
    h_in2[gx] = total
    await_bytes(h_in2.at[1:16], h_sem.at[3])
    total = h_in2[0]
    for k in range(1, 16):
        total = total + h_in2[k]

    gain = weights_v[...] * jnp.sqrt(1.0 + total)
    new = 1024.0 * gain / jnp.sum(gain)
    new_o[...] = new
    for k in range(8):
        sens_o[k] = jnp.sum(jnp.where(rank == float(k), total, 0.0))

    ids = ids_v[...]
    lane = lax.broadcasted_iota(jnp.int32, (128, 128), 1)
    picked = jnp.zeros((128, 128), f32)
    for k in range(8):
        picked = picked + jnp.where(ids == (lane + k * 128).astype(f32), new_o[k:k + 1, :], 0.0)
    wide[...] = jnp.broadcast_to(jnp.sum(picked, axis=1, keepdims=True), (128, 128))

    def weigh(i, acc):
        for u in range(8):
            slot = i * 8 + u
            acc = acc + wide[pl.ds(slot, 1), :] * dens[slot]
        return acc

    out = lax.fori_loop(0, 16, weigh, jnp.zeros((64, 128), f32))
    dens_o[:, :128] = out[:32]
    dens_o[:, 128:] = out[32:]

    for k in KINDS:
        await_bytes(send[k].at[0:28], sent.at[0, k])
        await_bytes(in1[k], sent.at[1, k])
        await_bytes(in2[k], sent.at[3, k])
        await_bytes(final[k], sent.at[2, k])
        await_bytes(metas.at[k, 0:4, 1:8], m_sem.at[0, k])
    await_bytes(h_in.at[1:8], h_sem.at[0])
    await_bytes(h_in2.at[1:16], h_sem.at[2])


def finish(sens, new, dens, sens_o, new_o, dens_o):
    for k in range(8):
        sens_o[k] = sens[k]
    new_o[...] = new[...]
    dens_o[...] = dens[...]


def local(probes, blk_rows, blk_sensor, blk_count, coef, owner, weights):
    tile_r, tile_c, probe_n = probes.shape
    nblk, foot = blk_rows.shape
    f32, bf16 = jnp.float32, jnp.bfloat16
    vmem = pl.BlockSpec(memory_space=pltpu.VMEM)
    smem = pl.BlockSpec(memory_space=pltpu.SMEM)
    anyw = pl.BlockSpec(memory_space=pl.ANY)
    dma = pltpu.SemaphoreType.DMA
    outs = (
        jax.ShapeDtypeStruct((8,), f32),
        jax.ShapeDtypeStruct((8, 128), f32),
        jax.ShapeDtypeStruct((tile_r, tile_c), f32),
    )
    sens, new, dens = pl.pallas_call(
        kernel,
        out_shape=outs,
        in_specs=[anyw, vmem, anyw] + [vmem] * 5,
        out_specs=(smem, vmem, vmem),
        scratch_shapes=[
            pltpu.SMEM((nblk * foot,), jnp.int32),
            pltpu.VMEM((tile_r * tile_c, probe_n), bf16),
            pltpu.VMEM((tile_r * tile_c, 2, 128), f32),
            pltpu.VMEM((3, 256, 128), f32),
            pltpu.VMEM((128, 2, 128), f32),
            pltpu.VMEM((5, 4, 8, 2, 128), f32),
            pltpu.VMEM((nblk, foot), f32),
            pltpu.VMEM((nblk, foot), f32),
            pltpu.VMEM((nblk, 64, 128), f32),
            pltpu.VMEM((8, probe_n), f32),
            pltpu.VMEM((256, 128), bf16),
            *[
                pltpu.VMEM((kinds, *dims, width), kind)
                for kinds, width in ((3, probe_n), (2, probe_n // 2))
                for dims, kind in (
                    ((32, nblk), bf16), ((4, 8, nblk), bf16), ((1024,), f32), ((2, 512), bf16), ((2, 512), bf16),
                    ((2, 1024), bf16), ((2, 1024), bf16), ((3, 256), bf16), ((3, 256), bf16),
                )
            ],
            pltpu.VMEM((8, 128), f32),
            pltpu.VMEM((8, 8, 128), f32),
            pltpu.VMEM((8, 128), f32),
            pltpu.VMEM((16, 8, 128), f32),
            pltpu.VMEM((128, 128), f32),
            dma((4,)), dma(()), dma((4, 5)), dma((5, 8)), dma((5, 2)), dma((5, 2)), dma((2, 5)), dma((5,)), dma((4,)),
        ],
        compiler_params=pltpu.CompilerParams(
            collective_id=0, has_side_effects=True, vmem_limit_bytes=60 * 2 ** 20
        ),
        name="exchange",
    )(
        blk_rows.reshape(-1), blk_count.reshape(1, 1), probes.reshape(tile_r * tile_c, probe_n), blk_rows, coef,
        blk_sensor.reshape(1, nblk), owner.reshape(8, 128), weights.reshape(8, 128),
    )
    sens, new, dens = pl.pallas_call(
        finish, out_shape=outs, in_specs=[smem, vmem, vmem], out_specs=(smem, vmem, vmem), name="finish",
    )(sens, new, dens)
    return sens, new.reshape(-1), dens


def solution(mesh):
    in_specs = (
        P("gx", "gy", None),
        P(("gx", "gy"), None),
        P(("gx", "gy")),
        P(("gx", "gy")),
        P(("gx", "gy"), None),
        P(),
        P(),
    )
    out_specs = (P(("gx", "gy")), P(), P("gx", "gy"))
    return jax.shard_map(local, mesh=mesh, in_specs=in_specs, out_specs=out_specs, check_vma=False)
```

```python
import jax
import jax.numpy as jnp
from jax import lax
from jax.experimental import pallas as pl
from jax.experimental.pallas import tpu as pltpu
from jax.sharding import PartitionSpec as P

MESH = pl.DeviceIdType.MESH
HIGHEST = lax.Precision.HIGHEST
FIRST = (0, 1, 2, 0, 2)
SECOND = (1, 2, 0, 1, 1)
THIRD = (2, 0, 1, 2, 0)
BASE = (0, 16, 32, 48, 48)
KINDS = (0, 1, 2, 3, 4)
TURN = {2: 0, 1: 1, 3: 2, 0: 3}


def place():
    gx, gy = lax.axis_index("gx"), lax.axis_index("gy")
    return [lax.rem(gx, 4), gx // 4, gy // 2], lax.rem(gy, 2)


def peer(axis, off, core_off):
    at, core = place()
    at[axis] = lax.rem(at[axis] + off, 4)
    return at[1] * 4 + at[0], at[2] * 2 + lax.rem(core + core_off, 2)


def order(i):
    return lax.rem(1 + 2 * i - 3 * (i // 2), 4)


def decode(pos):
    a, b = lax.rem(pos // 8, 2), pos // 16
    return 2 - a + b - 2 * a * b, order(lax.rem(pos, 4)), lax.rem(pos, 8) // 4


def kernel(
    rows_h, count_v, probes_h, rows_v, coef_b, ids_r, owner_v, weights_v,
    sens_o, new_o, dens_o,
    rows_s, probes, tile, stage, meta, metas, coef_v, ids_v, dens, dither, steps_v,
    send_w, zone_w, part_w, out1_w, in1_w, out2_w, in2_w, parcel_w, final_w,
    send_n, zone_n, part_n, out1_n, in1_n, out2_n, in2_n, parcel_n, final_n,
    h_send, h_in, h_mid, h_in2, wide,
    in_sem, row_sem, sent, rs1, r1_sem, r2_sem, m_sem, fr, h_sem,
):
    n_pts, probe_n = probes.shape
    foot = 128
    chunk = n_pts // 4
    gx, gy = lax.axis_index("gx"), lax.axis_index("gy")
    me = gx * 8 + gy
    at, core = place()
    bf16, f32 = jnp.bfloat16, jnp.float32

    def by_kind(wide_ref, narrow_ref):
        return [wide_ref.at[i] for i in range(3)] + [narrow_ref.at[i] for i in range(2)]

    send, zone, part = by_kind(send_w, send_n), by_kind(zone_w, zone_n), by_kind(part_w, part_n)
    out1, in1 = by_kind(out1_w, out1_n), by_kind(in1_w, in1_n)
    out2, in2 = by_kind(out2_w, out2_n), by_kind(in2_w, in2_n)
    parcel, final = by_kind(parcel_w, parcel_n), by_kind(final_w, final_n)
    lanes = [slice(0, 256)] * 3 + [slice(0, 128), slice(128, 256)]

    def load(i):
        part_of = pl.ds(i * chunk, chunk)
        return pltpu.make_async_copy(probes_h.at[part_of], probes.at[part_of], in_sem.at[i])

    rows_in = pltpu.make_async_copy(rows_h, rows_s, row_sem)
    for i in range(4):
        load(i).start()
    rows_in.start()
    barrier = pltpu.get_barrier_semaphore()

    def greet(device):
        pl.semaphore_signal(barrier, inc=1, device_id=device, device_id_type=MESH)

    for k in range(1, 16):
        greet((lax.rem(gx // 4 + k // 4, 4) * 4 + lax.rem(lax.rem(gx, 4) + k % 4, 4), gy))
    for k in range(1, 8):
        greet((gx, lax.rem(gy + k, 8)))
    for axis in (0, 1):
        for off in (1, 2, 3):
            greet(peer(axis, off, 1))

    flat = tile.reshape(2 * n_pts, 128)

    def widen(i, c):
        block = probes[pl.ds(pl.multiple_of(i * 64, 64), 64), :].astype(f32)
        flat[pl.ds(i * 128, 64, 2), :] = block[:, :128]
        flat[pl.ds(i * 128 + 1, 64, 2), :] = block[:, 128:]
        return c

    slot_of = lax.broadcasted_iota(jnp.int32, (128, 128), 0)
    coef_v[...] = jnp.where(slot_of < count_v[...], coef_b[...].astype(f32), 0.0)
    names_r = jnp.broadcast_to(ids_r[...].astype(f32), (128, 128))
    meta[:, 0, :] = coef_v[...].T
    meta[:, 1, :] = names_r
    ids_v[...] = names_r.T
    for i in range(4):
        load(i).wait()
        lax.fori_loop(i * (chunk // 64), (i + 1) * (chunk // 64), widen, 0)
    level = (
        lax.rem(lax.broadcasted_iota(jnp.int32, (8, probe_n), 1) * 97, probe_n).astype(f32) + 0.5
    ) * (1.0 / probe_n)
    bell = jnp.where(
        level < 0.5, jnp.sqrt(2.0 * level) - 1.0, 1.0 - jnp.sqrt(jnp.maximum(2.0 - 2.0 * level, 0.0))
    )
    dither[...] = 1.0 + bell * (1.0 / 128)
    rows_in.wait()
    for i in range(16):
        steps_v[i * 16:(i + 1) * 16, :] = (
            lax.broadcasted_iota(jnp.int32, (16, 128), 0) + i * 16
        ).astype(f32).astype(bf16)

    def meta1(k, of, oc):
        first = lax.rem(core + oc, 2) * 64 + BASE[k] + lax.rem(at[FIRST[k]] + of, 4) * 4
        src = oc * 4 + of
        return pltpu.make_async_remote_copy(
            src_ref=meta.at[pl.ds(first, 4)], dst_ref=metas.at[k, pl.ds(0, 4), src],
            send_sem=m_sem.at[0, k], recv_sem=m_sem.at[1, k],
            device_id=peer(FIRST[k], of, oc), device_id_type=MESH,
        )

    def copy1(k, pos):
        og, of, oc = decode(pos)
        return pltpu.make_async_remote_copy(
            src_ref=send[k].at[pos], dst_ref=zone[k].at[og, oc * 4 + of],
            send_sem=sent.at[0, k], recv_sem=rs1.at[k, pos // 4],
            device_id=peer(FIRST[k], of, oc), device_id_type=MESH,
        )

    def ring1(k, half):
        return pltpu.make_async_remote_copy(
            src_ref=out1[k].at[half], dst_ref=in1[k].at[half],
            send_sem=sent.at[1, k], recv_sem=r1_sem.at[k, half],
            device_id=peer(SECOND[k], 1 + 2 * half, 0), device_id_type=MESH,
        )

    def ring2(k, half):
        return pltpu.make_async_remote_copy(
            src_ref=out2[k].at[half], dst_ref=in2[k].at[half],
            send_sem=sent.at[3, k], recv_sem=r2_sem.at[k, half],
            device_id=peer(SECOND[k], 1 + 2 * half, 0), device_id_type=MESH,
        )

    def await_bytes(ref, sem):
        pltpu.make_async_copy(ref, ref, sem).wait()

    def copy3(k, oh):
        return pltpu.make_async_remote_copy(
            src_ref=parcel[k].at[oh - 1], dst_ref=final[k].at[oh - 1],
            send_sem=sent.at[2, k], recv_sem=fr.at[k],
            device_id=peer(THIRD[k], oh, 0), device_id_type=MESH,
        )

    others = [(of, oc) for oc in (0, 1) for of in (1, 3, 2, 0) if (of, oc) != (0, 0)]
    for k in KINDS:
        metas[k, 0:4, 0] = meta[pl.ds(core * 64 + BASE[k] + at[FIRST[k]] * 4, 4)]

    def gather(k, pos, buf):
        og, of, oc = decode(pos)
        chan = (
            lax.rem(core + oc, 2) * 64 + BASE[k]
            + lax.rem(at[FIRST[k]] + of, 4) * 4 + lax.rem(at[SECOND[k]] + og, 4)
        )
        for i in range(128):
            stage[buf, 2 * i:2 * i + 2, :] = tile[rows_s[chan + i * 128]]
        left = stage[buf, pl.ds(0, 128, 2), :].astype(bf16)
        right = stage[buf, pl.ds(1, 128, 2), :].astype(bf16)
        if k < 3:
            send[k][pos, :, :128] = left
            send[k][pos, :, 128:] = right
        else:
            send[3][pos] = left
            send[4][twin(pos)] = right

    def twin(pos):
        _, of, _ = decode(pos)
        of = lax.rem(of + at[0] - at[2] + 4, 4)
        a, b = lax.rem(of, 2), of // 2
        return pos // 4 * 4 + 3 - 3 * a - b + 2 * a * b

    def give(k, pos):
        mine = lax.rem(pos, 8) == 3

        @pl.when(mine)
        def _():
            og, _, _ = decode(pos)
            zone[k][og, 0] = send[k][pos]

        @pl.when(jnp.logical_not(mine))
        def _():
            copy1(k, pos).start()

    def first_loop(pos, c):
        for buf, k in enumerate((1, 2, 0)):
            gather(k, pos, buf)
            if buf == 0:
                @pl.when(pos == 1)
                def _():
                    pl.semaphore_wait(barrier, 28)
                    for of, oc in others:
                        for j in KINDS:
                            meta1(j, of, oc).start()

            @pl.when(pos > 0)
            def _():
                give(k, pos - 1)

        return c

    def second_loop(pos, c):
        gather(3, pos, 0)

        @pl.when(pos > 0)
        def _():
            give(3, pos - 1)
            give(4, twin(pos - 1))

        return c

    q = lax.broadcasted_iota(jnp.int32, (64, 128), 0)
    hi_of = jnp.where(q < 32, 2 * q, 2 * q - 63)
    lo_of = lax.broadcasted_iota(jnp.int32, (128, 128), 0)

    def spread(first):
        for u in range(4):
            row = rows_v[pl.ds(first + u, 1), :]
            val = coef_v[pl.ds(first + u, 1), :]
            high = jnp.where(row // 128 == hi_of, val, 0.0).astype(bf16)
            low = jnp.where(lax.rem(row, 128) == lo_of, val, 0.0).astype(bf16)
            dens[first + u] = lax.dot_general(
                high, low, (((1,), (1,)), ((), ())), preferred_element_type=f32
            )

    def spread_loop(i, c):
        spread(i * 4)
        return c

    def mix(k, og, into):
        turn = TURN[og]
        await_bytes(zone[k].at[og, 1:4], rs1.at[k, 2 * turn])
        await_bytes(zone[k].at[og, 4:8], rs1.at[k, 2 * turn + 1])
        chan = lax.rem(at[SECOND[k]] + og, 4)
        zero = jnp.zeros((16, 128), bf16)

        for m in range(4):
            total = None
            for oc in range(2):
                tags = [metas[k, chan, oc * 4 + u] for u in range(4)]
                vals = [jnp.broadcast_to(t[0:1], (16, 128)).astype(bf16) for t in tags]
                base = float(m * 256)
                names = [jnp.broadcast_to(t[1:2] - base, (16, 128)).astype(bf16) for t in tags]
                mixer = jnp.concatenate(
                    [
                        jnp.concatenate(
                            [
                                jnp.where(names[u] == steps_v[i * 16:(i + 1) * 16, :], vals[u], zero)
                                for i in range(16)
                            ],
                            axis=0,
                        )
                        for u in range(4)
                    ],
                    axis=1,
                )
                cols = zone[k][og, oc * 4:oc * 4 + 4].reshape(512, 256 if k < 3 else 128)
                got = jnp.dot(mixer, cols, preferred_element_type=f32)
                total = got if total is None else total + got
            into(m, total)

    def rows_at(m):
        return pl.ds(pl.multiple_of(m * 256, 256), 256)

    def step1(k):
        def into(m, total):
            out1[k][m // 2, m % 2 * 256:m % 2 * 256 + 256, :] = (
                total * dither[0:1, lanes[k]]
            ).astype(bf16)

        mix(k, 2, into)
        ring1(k, 0).start()
        ring1(k, 1).start()

    def step2(k):
        for half in (0, 1):
            def into(m, total):
                if m // 2 == half:
                    total = total + in1[k][half, m % 2 * 256:m % 2 * 256 + 256, :].astype(f32)
                out2[k][half, m * 256:m * 256 + 256, :] = (total * dither[0:1, lanes[k]]).astype(bf16)

            await_bytes(in1[k].at[half], r1_sem.at[k, half])
            mix(k, 1 + 2 * half, into)
            ring2(k, half).start()

    def own(k):
        def into(m, total):
            part[k][m * 256:m * 256 + 256, :] = total

        mix(k, 0, into)

    def collect(k):
        for half in (0, 1):
            await_bytes(in2[k].at[half], r2_sem.at[k, half])

    def summed(k, block):
        rows = part[k][rows_at(block), :]
        for half in (0, 1):
            rows = rows + in2[k][half, rows_at(block), :].astype(f32)
        return rows

    def sum_up(k):
        for oh in (1, 3, 2):
            rows = summed(k, lax.rem(at[THIRD[k]] + oh, 4))
            parcel[k][oh - 1] = (rows * dither[0:1, lanes[k]]).astype(bf16)
        for oh in (1, 3, 2):
            copy3(k, oh).start()

    lax.fori_loop(0, 32, first_loop, 0)
    for k in (1, 2, 0):
        give(k, 31)
    for k in KINDS:
        await_bytes(metas.at[k, 0:4, 1:8], m_sem.at[1, k])
    step1(0)
    step1(1)
    step1(2)
    lax.fori_loop(0, 32, second_loop, 0)
    give(3, 31)
    give(4, twin(31))
    step2(0)
    step2(1)
    step2(2)
    step1(3)
    step1(4)
    own(1)
    own(0)
    lax.fori_loop(0, 16, spread_loop, 0)
    own(2)
    lax.fori_loop(16, 32, spread_loop, 0)
    collect(0)
    sum_up(0)
    step2(3)
    step2(4)
    own(3)
    own(4)
    collect(1)
    sum_up(1)
    collect(2)
    sum_up(2)
    collect(3)
    sum_up(3)
    collect(4)
    sum_up(4)

    h_send[...] = jnp.zeros_like(h_send)
    ones = jnp.ones((8, 128), f32)
    for k in KINDS:
        await_bytes(final[k], fr.at[k])
        block = at[THIRD[k]]
        whole = summed(k, block)
        for i in range(3):
            whole = whole + final[k][i].astype(f32)
        whole = whole * whole
        if k < 3:
            whole = whole[:, :128] + whole[:, 128:]
        sums = lax.dot_general(
            ones, whole, (((1,), (1,)), ((), ())),
            preferred_element_type=f32, precision=HIGHEST,
        ) * (1.0 / (foot * probe_n))
        for i in range(2):
            h_send[pl.ds(2 * block + i, 1), :] += sums[0:1, i * 128:(i + 1) * 128]

    def first_copy(k):
        to = lax.rem(gy + k, 8)
        return pltpu.make_async_remote_copy(
            src_ref=h_send, dst_ref=h_in.at[gy],
            send_sem=h_sem.at[0], recv_sem=h_sem.at[1],
            device_id=(gx, to), device_id_type=MESH,
        )

    def second_copy(k):
        to = lax.rem(gx // 4 + k // 4, 4) * 4 + lax.rem(lax.rem(gx, 4) + k % 4, 4)
        return pltpu.make_async_remote_copy(
            src_ref=h_mid, dst_ref=h_in2.at[gx],
            send_sem=h_sem.at[2], recv_sem=h_sem.at[3],
            device_id=(to, gy), device_id_type=MESH,
        )

    for k in (5, 4, 3, 7, 2, 6, 1):
        first_copy(k).start()
    h_in[gy] = h_send[...]
    mine = owner_v[...] == me
    count = jnp.where(mine, 1.0, 0.0)
    before = jnp.where(
        lax.broadcasted_iota(jnp.int32, (128, 128), 0) < lax.broadcasted_iota(jnp.int32, (128, 128), 1),
        1.0, 0.0,
    )
    above = jnp.where(
        lax.broadcasted_iota(jnp.int32, (8, 8), 1) < lax.broadcasted_iota(jnp.int32, (8, 8), 0),
        1.0, 0.0,
    )
    in_row = jnp.dot(count, before, precision=HIGHEST, preferred_element_type=f32)
    rank = in_row + jnp.dot(
        above, jnp.broadcast_to(jnp.sum(count, axis=1, keepdims=True), (8, 128)),
        precision=HIGHEST, preferred_element_type=f32,
    )
    rank = jnp.where(mine, rank, -1.0)
    await_bytes(h_in.at[1:8], h_sem.at[1])
    total = h_in[0]
    for k in range(1, 8):
        total = total + h_in[k]
    h_mid[...] = total
    for k in (10, 6, 14, 9, 11, 2, 8, 5, 15, 7, 13, 1, 3, 4, 12):
        second_copy(k).start()
    h_in2[gx] = total
    await_bytes(h_in2.at[1:16], h_sem.at[3])
    total = h_in2[0]
    for k in range(1, 16):
        total = total + h_in2[k]

    gain = weights_v[...] * jnp.sqrt(1.0 + total)
    new = 1024.0 * gain / jnp.sum(gain)
    new_o[...] = new
    for k in range(8):
        sens_o[k] = jnp.sum(jnp.where(rank == float(k), total, 0.0))

    ids = ids_v[...]
    lane = lax.broadcasted_iota(jnp.int32, (128, 128), 1)
    picked = jnp.zeros((128, 128), f32)
    for k in range(8):
        picked = picked + jnp.where(ids == (lane + k * 128).astype(f32), new_o[k:k + 1, :], 0.0)
    wide[...] = jnp.broadcast_to(jnp.sum(picked, axis=1, keepdims=True), (128, 128))

    def weigh(i, acc):
        for u in range(8):
            slot = i * 8 + u
            acc = acc + wide[pl.ds(slot, 1), :] * dens[slot]
        return acc

    out = lax.fori_loop(0, 16, weigh, jnp.zeros((64, 128), f32))
    dens_o[:, :128] = out[:32]
    dens_o[:, 128:] = out[32:]

    for k in KINDS:
        await_bytes(send[k].at[0:28], sent.at[0, k])
        await_bytes(in1[k], sent.at[1, k])
        await_bytes(in2[k], sent.at[3, k])
        await_bytes(final[k], sent.at[2, k])
        await_bytes(metas.at[k, 0:4, 1:8], m_sem.at[0, k])
    await_bytes(h_in.at[1:8], h_sem.at[0])
    await_bytes(h_in2.at[1:16], h_sem.at[2])


def finish(sens, new, dens, sens_o, new_o, dens_o):
    for k in range(8):
        sens_o[k] = sens[k]
    new_o[...] = new[...]
    dens_o[...] = dens[...]


def local(probes, blk_rows, blk_sensor, blk_count, coef, owner, weights):
    tile_r, tile_c, probe_n = probes.shape
    nblk, foot = blk_rows.shape
    f32, bf16 = jnp.float32, jnp.bfloat16
    vmem = pl.BlockSpec(memory_space=pltpu.VMEM)
    smem = pl.BlockSpec(memory_space=pltpu.SMEM)
    anyw = pl.BlockSpec(memory_space=pl.ANY)
    dma = pltpu.SemaphoreType.DMA
    outs = (
        jax.ShapeDtypeStruct((8,), f32),
        jax.ShapeDtypeStruct((8, 128), f32),
        jax.ShapeDtypeStruct((tile_r, tile_c), f32),
    )
    sens, new, dens = pl.pallas_call(
        kernel,
        out_shape=outs,
        in_specs=[anyw, vmem, anyw] + [vmem] * 5,
        out_specs=(smem, vmem, vmem),
        scratch_shapes=[
            pltpu.SMEM((nblk * foot,), jnp.int32),
            pltpu.VMEM((tile_r * tile_c, probe_n), bf16),
            pltpu.VMEM((tile_r * tile_c, 2, 128), f32),
            pltpu.VMEM((3, 256, 128), f32),
            pltpu.VMEM((128, 2, 128), f32),
            pltpu.VMEM((5, 4, 8, 2, 128), f32),
            pltpu.VMEM((nblk, foot), f32),
            pltpu.VMEM((nblk, foot), f32),
            pltpu.VMEM((nblk, 64, 128), f32),
            pltpu.VMEM((8, probe_n), f32),
            pltpu.VMEM((256, 128), bf16),
            *[
                pltpu.VMEM((kinds, *dims, width), kind)
                for kinds, width in ((3, probe_n), (2, probe_n // 2))
                for dims, kind in (
                    ((32, nblk), bf16), ((4, 8, nblk), bf16), ((1024,), f32), ((2, 512), bf16), ((2, 512), bf16),
                    ((2, 1024), bf16), ((2, 1024), bf16), ((3, 256), bf16), ((3, 256), bf16),
                )
            ],
            pltpu.VMEM((8, 128), f32),
            pltpu.VMEM((8, 8, 128), f32),
            pltpu.VMEM((8, 128), f32),
            pltpu.VMEM((16, 8, 128), f32),
            pltpu.VMEM((128, 128), f32),
            dma((4,)), dma(()), dma((4, 5)), dma((5, 8)), dma((5, 2)), dma((5, 2)), dma((2, 5)), dma((5,)), dma((4,)),
        ],
        compiler_params=pltpu.CompilerParams(
            collective_id=0, has_side_effects=True, vmem_limit_bytes=60 * 2 ** 20
        ),
        name="exchange",
    )(
        blk_rows.reshape(-1), blk_count.reshape(1, 1), probes.reshape(tile_r * tile_c, probe_n), blk_rows, coef,
        blk_sensor.reshape(1, nblk), owner.reshape(8, 128), weights.reshape(8, 128),
    )
    sens, new, dens = pl.pallas_call(
        finish, out_shape=outs, in_specs=[smem, vmem, vmem], out_specs=(smem, vmem, vmem), name="finish",
    )(sens, new, dens)
    return sens, new.reshape(-1), dens


def solution(mesh):
    in_specs = (
        P("gx", "gy", None),
        P(("gx", "gy"), None),
        P(("gx", "gy")),
        P(("gx", "gy")),
        P(("gx", "gy"), None),
        P(),
        P(),
    )
    out_specs = (P(("gx", "gy")), P(), P("gx", "gy"))
    return jax.shard_map(local, mesh=mesh, in_specs=in_specs, out_specs=out_specs, check_vma=False)
```
